128 devices in a mesh: ha: 4 (over z_lo, core), wa: 4 (over y), hd: 8 (over z_hi, x).
Axes of the slice: x: 4, y: 4, z: 4 (z_hi: 2, z_lo: 2; z = z_hi * 2 + z_lo), core: 2. Of those that a mesh axis runs over, the one named last changes fastest.
Arguments:
- queries: bfloat16 [12, 32, 64, 3072], P(None, 'ha', 'wa', 'hd'), may hold values from -10 to 10
- video_keys: bfloat16 [12, 32, 64, 3072], P(None, 'ha', 'wa', 'hd'), may hold values from -5 to 5
- video_values: bfloat16 [12, 32, 64, 3072], P(None, 'ha', 'wa', 'hd'), may hold values from -6 to 6
- text_keys: bfloat16 [256, 3072], P(None, 'hd'), may hold values from -5 to 5
- text_values: bfloat16 [256, 3072], P(None, 'hd'), may hold values from -6 to 6
- tile_radius: int32 [3, 2, 4, 8], P(None, None, 'ha', 'wa'), may hold values from 0 to 1, as said below
- out_weight: bfloat16 [3072, 3072], P('hd'), may hold values from -0.875 to 0.875
Outputs:
- projected: bfloat16 [12, 32, 64, 3072], P(None, 'ha', 'wa', 'hd')
The draws below stay inside these ranges and needn't reach their ends.
Inputs may be any that keep to these rules, and one draw needn't show every extreme that they name: `tile_radius`: every video query has a window of at most one tile in each direction; some tile has radius 1 in all three.
All inputs are finite; a program needn't handle non-finite values.
Results may differ from the reference program's by a relative error of at most 0.012.
Values may be sent and summed in bfloat16 or wider, within the bound.
A program may use at most 192 MiB of HBM per device.

```python
import jax
import jax.numpy as jnp
from jax import lax

HEADS = 24
HEAD = 128
D = 3072
TEXT = 256
TILE_T = 6
TILE_H = 8
TILE_W = 8
TT_TILES = 2
FRAMES = 12
ROW_TILES = 4
COL_TILES = 8
HEIGHT = 32
WIDTH = 64
N_HD = 8


def paired_draw(key):
    base = jax.random.fold_in(key, 71)
    shape = (FRAMES, HEIGHT, WIDTH, HEADS * HEAD)
    first = jax.random.normal(jax.random.fold_in(base, 1), shape, jnp.float32)
    second = jax.random.normal(jax.random.fold_in(base, 2), shape, jnp.float32)
    q_part = jnp.clip(2.0 * first, -10.0, 10.0)
    k_part = jnp.clip(second, -5.0, 5.0)
    return (q_part, k_part)


def draw_queries(key, part):
    return paired_draw(key)[0].astype(jnp.bfloat16)


def draw_video_keys(key, part):
    return paired_draw(key)[1].astype(jnp.bfloat16)


def draw_tile_radius(key, part):
    drawn = jax.random.randint(key, (3, TT_TILES, ROW_TILES, COL_TILES), 0, 2).astype(jnp.int32)
    return drawn.at[:, 0, 0, 0].set(1)


def block_scale(key, extent, cuts, least, high):
    def one(dim, parts):
        draws = jax.random.uniform(jax.random.fold_in(jax.random.fold_in(key, 6), dim), (parts,), jnp.float32, least / len(cuts), high / len(cuts))
        return jnp.repeat(jnp.exp(draws), extent[dim] // parts).reshape((-1,) + (1,) * (len(extent) - dim - 1))

    factor_of = one(*cuts[0])
    for cut in cuts[1:]:
        factor_of = factor_of * one(*cut)
    return factor_of


def noise(key, shape, deviation, most, cuts=(), kind=jnp.bfloat16):
    values = jax.random.normal(key, shape, jnp.float32) * deviation
    if len(cuts) > 0:
        values = block_scale(key, shape, cuts, -0.22, 0.18) * values
    return jnp.clip(values, min=-most, max=most).astype(kind)


def setup_inputs(seed: int = 0) -> dict:
    key_of = jax.random.split(jax.random.key(seed), 8)
    return {
        "queries": draw_queries(jax.random.fold_in(key_of[7], 71), 0),
        "video_keys": draw_video_keys(jax.random.fold_in(key_of[7], 71), 0),
        "video_values": noise(key_of[2], (FRAMES, HEIGHT, WIDTH, HEADS * HEAD), 1.0, 6.0, ((1, 4), (2, 4), (3, 8))),
        "text_keys": noise(key_of[3], (TEXT, HEADS * HEAD), 1.0, 5.0, ((1, 8),)),
        "text_values": noise(key_of[4], (TEXT, HEADS * HEAD), 1.0, 6.0, ((1, 8),)),
        "tile_radius": draw_tile_radius(jax.random.fold_in(key_of[7], 71), 0),
        "out_weight": noise(key_of[6], (HEADS * HEAD, D), 48 ** -0.5, 0.875, ((0, 8),)),
    }


def reference(queries, video_keys, video_values, text_keys, text_values, tile_radius, out_weight):
    n_frames, n_height, n_width, channels = queries.shape
    time_tiles = n_frames // TILE_T
    row_tiles = n_height // TILE_H
    col_tiles = n_width // TILE_W
    head_count = channels // HEAD
    factor = HEAD ** -0.5
    padding = ((0, 0), (TILE_H, TILE_H), (TILE_W, TILE_W), (0, 0))
    keys_padded = jnp.pad(video_keys, padding)
    values_padded = jnp.pad(video_values, padding)
    text_key32 = text_keys.astype(jnp.float32).reshape(-1, head_count, HEAD)
    text_val32 = text_values.astype(jnp.float32).reshape(-1, head_count, HEAD)

    def one_tile(tile_index):
        time_tile = tile_index // (row_tiles * col_tiles)
        row_tile = (tile_index // col_tiles) % row_tiles
        col_tile = tile_index % col_tiles
        zero = jnp.zeros((), jnp.int32)
        q_tile = lax.dynamic_slice(queries, (time_tile * TILE_T, row_tile * TILE_H, col_tile * TILE_W, zero), (TILE_T, TILE_H, TILE_W, channels))
        q_tile = q_tile.astype(jnp.float32).reshape(-1, head_count, HEAD)
        k_tile = lax.dynamic_slice(keys_padded, (zero, row_tile * TILE_H, col_tile * TILE_W, zero), (n_frames, 3 * TILE_H, 3 * TILE_W, channels))
        v_tile = lax.dynamic_slice(values_padded, (zero, row_tile * TILE_H, col_tile * TILE_W, zero), (n_frames, 3 * TILE_H, 3 * TILE_W, channels))
        k_tile = k_tile.astype(jnp.float32).reshape(-1, head_count, HEAD)
        v_tile = v_tile.astype(jnp.float32).reshape(-1, head_count, HEAD)
        key_time = jnp.arange(n_frames, dtype=jnp.int32) // TILE_T
        key_row = row_tile - 1 + jnp.arange(3 * TILE_H, dtype=jnp.int32) // TILE_H
        key_col = col_tile - 1 + jnp.arange(3 * TILE_W, dtype=jnp.int32) // TILE_W
        radius_here = tile_radius[:, time_tile, row_tile, col_tile]
        time_ok = jnp.abs(key_time - time_tile) <= radius_here[0]
        row_ok = (jnp.abs(key_row - row_tile) <= radius_here[1]) & (key_row >= 0) & (key_row < row_tiles)
        col_ok = (jnp.abs(key_col - col_tile) <= radius_here[2]) & (key_col >= 0) & (key_col < col_tiles)
        allowed = (time_ok[:, None, None] & row_ok[None, :, None] & col_ok[None, None, :]).reshape(-1)
        scores = jnp.einsum("qhd,khd->hqk", q_tile, k_tile) * factor
        text_scores = jnp.einsum("qhd,khd->hqk", q_tile, text_key32) * factor
        row_peak = jnp.maximum(jnp.max(jnp.where(allowed[None, None, :], scores, -jnp.inf), axis=2), jnp.max(text_scores, axis=2))[:, :, None]
        weights = jnp.where(allowed[None, None, :], jnp.exp(scores - row_peak), 0.0)
        text_weights = jnp.exp(text_scores - row_peak)
        row_total = jnp.sum(weights, axis=2) + jnp.sum(text_weights, axis=2)
        weights_low = lax.optimization_barrier(weights.astype(jnp.bfloat16)).astype(jnp.float32)
        text_low = lax.optimization_barrier(text_weights.astype(jnp.bfloat16)).astype(jnp.float32)
        numerator = jnp.einsum("hqk,khd->qhd", weights_low, v_tile) + jnp.einsum("hqk,khd->qhd", text_low, text_val32)
        result = (numerator / jnp.transpose(row_total)[:, :, None]).astype(jnp.bfloat16)
        return result.reshape(TILE_T, TILE_H, TILE_W, channels)

    tiles = lax.map(one_tile, jnp.arange(time_tiles * row_tiles * col_tiles, dtype=jnp.int32))
    tiles = tiles.reshape(time_tiles, row_tiles, col_tiles, TILE_T, TILE_H, TILE_W, channels)
    attended = jnp.transpose(tiles, (0, 3, 1, 4, 2, 5, 6)).reshape(-1, channels)
    group_width = channels // N_HD
    summed = jnp.zeros((attended.shape[0], out_weight.shape[1]), jnp.float32)
    for group in range(N_HD):
        portion = jnp.dot(attended[:, group * group_width:(group + 1) * group_width], out_weight[group * group_width:(group + 1) * group_width], preferred_element_type=jnp.float32)
        summed = summed + lax.optimization_barrier(portion.astype(jnp.bfloat16)).astype(jnp.float32)
    return summed.astype(jnp.bfloat16).reshape(n_frames, n_height, n_width, -1)
```

```python
import functools

import jax
import jax.numpy as jnp
from jax import lax
from jax.experimental import pallas as pl
from jax.experimental.pallas import tpu as pltpu
from jax.sharding import PartitionSpec as P

HEAD = 128
TILE_T = 6
TILE_H = 8
TILE_W = 8
FACTOR = 1.4426950408889634 * HEAD ** (-0.5)
FAR = 1e30
SUB = 256


def summed_on_arrival(value, axis, dim):
    size = lax.axis_size(axis)
    shape = value.shape
    blocks = value.reshape(*shape[:dim], size, shape[dim] // size, *shape[dim + 1 :])
    blocks = jnp.moveaxis(blocks, dim, 0)
    arrived = lax.all_to_all(blocks, axis, split_axis=0, concat_axis=0, tiled=True)
    return arrived.astype(jnp.float32).sum(axis=0)


def tiled(block):
    frames, height, across, channels = block.shape
    cols = across // TILE_W
    heads = channels // HEAD
    cut = block.reshape(frames, height, cols, TILE_W, heads, HEAD)
    return cut.transpose(4, 2, 0, 1, 3, 5).reshape(heads, cols, -1, HEAD)


def untiled(tiles, frames, height):
    cols, _, channels = tiles.shape
    cut = tiles.reshape(cols, frames, height, TILE_W, channels)
    return cut.transpose(1, 2, 0, 3, 4).reshape(frames, height, cols * TILE_W, channels)


def fold_chunk(q, k, v, pens, m_ref, l_ref, acc_ref, first=False):
    count = len(pens)
    keys = k.shape[0] // count
    for start in range(0, q.shape[0], SUB):
        at = slice(start, start + SUB)
        s = FACTOR * lax.dot_general(
            k, q[at], (((1,), (1,)), ((), ())), preferred_element_type=jnp.float32
        )
        parts = [s[i * keys : (i + 1) * keys] for i in range(count)]
        tops = [jnp.max(part, axis=0, keepdims=True) for part in parts]
        rows = [None if pen is None else pen[:, at] for pen in pens]
        tops = [top if row is None else top - row for top, row in zip(tops, rows)]
        m_new = functools.reduce(jnp.maximum, tops)
        if not first:
            m_old = m_ref[:, at]
            m_new = jnp.maximum(m_new, m_old)
        weights = [
            jnp.exp2(part - (m_new if row is None else m_new + row))
            for part, row in zip(parts, rows)
        ]
        total = functools.reduce(
            jnp.add, [jnp.sum(weight, axis=0, keepdims=True) for weight in weights]
        )
        low = [weight.astype(jnp.bfloat16) for weight in weights]
        low = low[0] if count == 1 else jnp.concatenate(low, axis=0)
        add = lax.dot_general(
            v, low, (((0,), (0,)), ((), ())), preferred_element_type=jnp.float32
        )
        if first:
            l_ref[:, at] = total
            acc_ref[:, at] = add
        else:
            shrink = jnp.exp2(m_old - m_new)
            l_ref[:, at] = l_ref[:, at] * shrink + total
            acc_ref[:, at] = acc_ref[:, at] * shrink + add
        m_ref[:, at] = m_new


def attend_kernel(radius, q_ref, kv_ref, tk_ref, tv_ref, out_ref, m_ref, l_ref, acc_ref):
    col = pl.program_id(1)
    ha, wa = lax.axis_index("ha"), lax.axis_index("wa")
    rows, cols = lax.axis_size("ha"), 2 * lax.axis_size("wa")
    q = q_ref[0, 0]
    fold_chunk(q, tk_ref[...], tv_ref[...], [None], m_ref, l_ref, acc_ref, first=True)
    late = lax.broadcasted_iota(jnp.int32, (1, q.shape[0]), 1) >= q.shape[0] // 2

    def visit(i, carry):
        row, gap = i // 3, i % 3
        key_row, key_col = ha + row - 1, 2 * wa + col + gap - 1
        there = (key_row >= 0) & (key_row < rows) & (key_col >= 0) & (key_col < cols)
        seen = []
        for t in range(2):
            seen.append(
                there
                & (jnp.abs(row - 1) <= radius[2 + t, col])
                & (jnp.abs(gap - 1) <= radius[4 + t, col])
            )

        @pl.when(seen[0] | seen[1])
        def _():
            pens = []
            for kt in range(2):
                pen = []
                for qt in range(2):
                    ok = seen[qt] & (abs(qt - kt) <= radius[qt, col])
                    pen.append(jnp.where(ok, 0.0, FAR))
                pens.append(jnp.where(late, pen[1], pen[0]))
            kv = kv_ref.at[row, col + gap, 0]
            fold_chunk(q, kv[0], kv[1], pens, m_ref, l_ref, acc_ref)

        return carry

    lax.fori_loop(0, 9, visit, 0)
    out_ref[0] = (acc_ref[...] / l_ref[...]).T.astype(out_ref.dtype)


def attend(radius, q, kv, text_keys, text_values):
    heads, cols, tokens, _ = q.shape
    grid = (heads, cols)
    return pl.pallas_call(
        attend_kernel,
        grid_spec=pltpu.PrefetchScalarGridSpec(
            num_scalar_prefetch=1,
            grid=grid,
            in_specs=[
                pl.BlockSpec((1, 1, tokens, HEAD), lambda h, c, r: (h, c, 0, 0)),
                pl.BlockSpec((3, 4, 1, 2, tokens, HEAD), lambda h, c, r: (0, 0, h, 0, 0, 0)),
                pl.BlockSpec((text_keys.shape[0], HEAD), lambda h, c, r: (0, h)),
                pl.BlockSpec((text_keys.shape[0], HEAD), lambda h, c, r: (0, h)),
            ],
            out_specs=pl.BlockSpec((1, tokens, HEAD), lambda h, c, r: (c, 0, h)),
            scratch_shapes=[
                pltpu.VMEM((1, tokens), jnp.float32),
                pltpu.VMEM((1, tokens), jnp.float32),
                pltpu.VMEM((HEAD, tokens), jnp.float32),
            ],
        ),
        out_shape=jax.ShapeDtypeStruct((cols, tokens, heads * HEAD), jnp.bfloat16),
        compiler_params=pltpu.CompilerParams(vmem_limit_bytes=56 * 1024 * 1024),
        cost_estimate=pl.CostEstimate(
            flops=20_000_000_000, bytes_accessed=18_000_000, transcendentals=30_000_000
        ),
        name="attend",
    )(radius, q, kv, text_keys, text_values)


def shifts(block, axis):
    count = lax.axis_size(axis)
    forward = [(i, i + 1) for i in range(count - 1)]
    backward = [(i + 1, i) for i in range(count - 1)]
    return lax.ppermute(block[0], axis, forward), lax.ppermute(block[1], axis, backward)


def shards(queries, video_keys, video_values, text_keys, text_values, tile_radius, out_weight):
    n_frames, height, across, channels = queries.shape
    q = tiled(queries)
    kv = jnp.stack([tiled(video_keys), tiled(video_values)], axis=2)
    kv = jnp.moveaxis(kv, 1, 0)
    left, right = shifts((kv[1:], kv[:1]), "wa")
    row = jnp.concatenate([left, kv, right], axis=0)
    above, below = shifts((row, row), "ha")
    window = jnp.stack([above, row, below])
    radius = tile_radius[:, :, 0, :].reshape(6, -1)
    mixture = attend(radius, q, window, text_keys, text_values)
    portion = jnp.dot(mixture.reshape(-1, channels), out_weight, preferred_element_type=jnp.float32)
    portion = portion.astype(jnp.bfloat16).reshape(across // TILE_W, -1, out_weight.shape[1])
    summed = summed_on_arrival(portion, "hd", 2).astype(jnp.bfloat16)
    return untiled(summed, n_frames, height)


def solution(mesh):
    placed = (
        P(None, "ha", "wa", "hd"),
        P(None, "ha", "wa", "hd"),
        P(None, "ha", "wa", "hd"),
        P(None, "hd"),
        P(None, "hd"),
        P(None, None, "ha", "wa"),
        P("hd", None),
    )
    return jax.shard_map(
        shards, mesh=mesh, in_specs=placed, out_specs=P(None, "ha", "wa", "hd"), check_vma=False
    )
```

```python
import functools

import jax
import jax.numpy as jnp
from jax import lax
from jax.experimental import pallas as pl
from jax.experimental.pallas import tpu as pltpu
from jax.sharding import PartitionSpec as P

HEAD = 128
TILE_W = 8
FACTOR = 1.4426950408889634 * HEAD ** (-0.5)
FAR = 1e30
SUB = 256
NX = 4
BF16 = jnp.bfloat16
F32 = jnp.float32
MESH = pl.DeviceIdType.MESH


def tiled(block):
    frames, height, across, channels = block.shape
    cols = across // TILE_W
    heads = channels // HEAD
    cut = block.reshape(frames, height, cols, TILE_W, heads, HEAD)
    return cut.transpose(4, 2, 0, 1, 3, 5).reshape(heads, cols, -1, HEAD)


def untiled(tiles, frames, height):
    cols, _, channels = tiles.shape
    cut = tiles.reshape(cols, frames, height, TILE_W, channels)
    return cut.transpose(1, 2, 0, 3, 4).reshape(frames, height, cols * TILE_W, channels)


def product(a, b, over_a, over_b):
    return lax.dot_general(a, b, (((over_a,), (over_b,)), ((), ())), preferred_element_type=F32)


def fold_chunk(q2, k, v, pens, m_ref, l_ref, acc_ref, s_ref, first=False):
    count = len(pens)
    keys = k.shape[0] // count
    k2 = jnp.concatenate([k, k], axis=1)
    for part, start in enumerate(range(0, q2.shape[0], SUB)):
        at = slice(start, start + SUB)
        s = product(k2, q2[at], 1, 1)
        held = s_ref.at[part]
        held[: k.shape[0]] = s
        tops = [
            jnp.max(s[i * keys : (i + 1) * keys], axis=0, keepdims=True) for i in range(count)
        ]
        rows = [None if pen is None else pen[:, at] for pen in pens]
        tops = [top if row is None else top - row for top, row in zip(tops, rows)]
        m_new = functools.reduce(jnp.maximum, tops)
        if not first:
            m_old = m_ref[:, at]
            m_new = jnp.maximum(m_new, m_old)
        weights = [
            jnp.exp2(held[i * keys : (i + 1) * keys] - (m_new if row is None else m_new + row))
            for i, row in enumerate(rows)
        ]
        total = functools.reduce(
            jnp.add, [jnp.sum(weight, axis=0, keepdims=True) for weight in weights]
        )
        low = [weight.astype(BF16) for weight in weights]
        low = low[0] if count == 1 else jnp.concatenate(low, axis=0)
        add = product(v, low, 0, 0)
        if first:
            l_ref[:, at] = total
            acc_ref[:, at] = add
        else:
            shrink = jnp.exp2(m_old - m_new)
            l_ref[:, at] = l_ref[:, at] * shrink + total
            acc_ref[:, at] = acc_ref[:, at] * shrink + add
        m_ref[:, at] = m_new


def layer_kernel(
    radius, q_ref, kv_ref, tk_ref, tv_ref, w_ref, out_ref,
    kvh, q2, m_ref, l_ref, acc_ref, s_ref, ag, wg, part, leave, arrive,
    row_s, row_r, par_s, par_r, z_s, z_r, parcol_s, parcol_r, zcol_s, zcol_r,
    w_s, w_r, wf_s, wf_r, wl, ag_s, ag_r, agf_s, agf_r, sum_s, sum_r,
):
    heads = q_ref.shape[0]
    tokens = q_ref.shape[2]
    width = heads * HEAD
    half = width // 2
    ha, wa, hd = lax.axis_index("ha"), lax.axis_index("wa"), lax.axis_index("hd")
    last = lax.axis_size("wa") - 1
    core = lax.rem(ha, 2)
    partner = ha + 1 - 2 * core
    inner = (ha == 1) | (ha == 2)
    peer = 3 - ha
    x = lax.rem(hd, NX)
    z = hd // NX
    near = 2 - 2 * core
    far = 2 * core
    has_left, has_right = wa > 0, wa < last

    def x_at(step):
        return z * NX + lax.rem(x + step, NX)

    def remote(src, dst, send, recv, device):
        return pltpu.make_async_remote_copy(
            src_ref=src, dst_ref=dst, send_sem=send, recv_sem=recv,
            device_id=device, device_id_type=MESH,
        )

    def row_copy(h, side):
        return remote(
            kv_ref.at[h, 1 - side], kvh.at[h, 1, 3 * side], row_s.at[h, side], row_r.at[h, side],
            {"wa": wa + 1 - 2 * side},
        )

    def par_copy(h):
        return remote(
            kv_ref.at[h], kvh.at[h, far, pl.ds(1, 2)], par_s.at[h], par_r.at[h], {"ha": partner}
        )

    def z_copy(h):
        return remote(
            kv_ref.at[h], kvh.at[h, near, pl.ds(1, 2)], z_s.at[h], z_r.at[h], {"ha": peer}
        )

    def parcol_copy(h, side):
        return remote(
            kvh.at[h, 1, 3 * side], kvh.at[h, far, 3 * side],
            parcol_s.at[h, side], parcol_r.at[h, side], {"ha": partner},
        )

    def zcol_copy(h, side):
        return remote(
            kvh.at[h, far, 2 - side], kvh.at[h, far, 3 * side],
            zcol_s.at[h, side], zcol_r.at[h, side], {"wa": wa + 1 - 2 * side},
        )

    def w_copy(step, zc):
        cols = pl.multiple_of((zc * NX + lax.rem(x + step, NX)) * width, HEAD)
        return remote(
            w_ref.at[pl.ds(core * half, half), pl.ds(cols, width)],
            wg.at[zc, pl.ds(x * width + core * half, half)],
            w_s.at[step - 1, zc], w_r.at[step - 1, zc], {"hd": x_at(step)},
        )

    def w_forward(step, zc):
        rows = pl.ds(lax.rem(x + NX - step, NX) * width + core * half, half)
        return remote(
            wg.at[zc, rows], wg.at[zc, rows],
            wf_s.at[step - 1, zc], wf_r.at[step - 1, zc], {"ha": partner},
        )

    def w_own(zc):
        cols = pl.multiple_of((zc * NX + x) * width, HEAD)
        return pltpu.make_async_copy(
            w_ref.at[:, pl.ds(cols, width)], wg.at[zc, pl.ds(x * width, width)], wl.at[zc]
        )

    def ag_copy(c, h, way):
        return remote(
            ag.at[c, x, h], ag.at[c, x, h], ag_s.at[c, h, way], ag_r.at[c, h, way],
            {"hd": x_at(1 + 2 * way)},
        )

    def ag_forward(c, h):
        block = ag.at[c, lax.rem(x + NX - 1 + 2 * c, NX), h]
        return remote(
            block, block, agf_s.at[c, h], agf_r.at[c, h], {"hd": x_at(1 + 2 * c)}
        )

    def sum_copy(c, b):
        at = pl.ds(b * SUB, SUB)
        return remote(
            leave.at[c, at], arrive.at[c, at], sum_s.at[c, b], sum_r.at[c, b],
            {"hd": lax.rem(hd + NX, 2 * NX)},
        )

    barrier = pltpu.get_barrier_semaphore()

    def greet(device):
        pl.semaphore_signal(barrier, inc=1, device_id=device, device_id_type=MESH)

    pl.when(has_left)(lambda: greet({"wa": wa - 1}))
    pl.when(has_right)(lambda: greet({"wa": wa + 1}))
    pl.when(inner)(lambda: greet({"ha": peer}))
    greet({"ha": partner})
    for step in range(1, NX):
        greet({"hd": x_at(step)})
    greet({"hd": lax.rem(hd + NX, 2 * NX)})
    pl.semaphore_wait(
        barrier,
        2 + NX - 1
        + has_left.astype(jnp.int32) + has_right.astype(jnp.int32) + inner.astype(jnp.int32),
    )

    def when_side(side, act):
        pl.when(has_right if side == 0 else has_left)(act)

    def when_from(side, act):
        pl.when(has_left if side == 0 else has_right)(act)

    def start_rows(h):
        for side in range(2):
            when_side(side, lambda side=side: row_copy(h, side).start())

    start_rows(0)
    for h in range(heads):
        pl.when(inner)(lambda h=h: z_copy(h).start())
        par_copy(h).start()
    for zc in range(2):
        w_own(zc).start()
        for step in (1, 3, 2):
            w_copy(step, zc).start()
    for h in range(heads):
        kvh[h, 1, 1:3] = kv_ref[h]

    def serve(h):
        for side in range(2):
            when_from(side, lambda side=side: row_copy(h, side).wait_recv())
        pl.when(inner)(lambda: z_copy(h).wait_recv())
        for side in range(2):
            when_from(side, lambda side=side: parcol_copy(h, side).start())
        for side in range(2):

            @pl.when(inner & (has_right if side == 0 else has_left))
            def _():
                zcol_copy(h, side).start()

        pl.when(h < heads - 1)(lambda: start_rows(h + 1))

    late = lax.broadcasted_iota(jnp.int32, (1, tokens), 1) >= tokens // 2
    n_rows = 2 + inner.astype(jnp.int32)

    def forward(c, h):
        ag_copy(c, h, c).wait_recv()
        ag_forward(c, h).start()

    def project(c):
        for h in range(heads):
            ag_copy(c, h, 1 - c).wait_recv()
            ag_forward(c, h).wait_recv()
        for b in range(tokens // SUB):
            at = slice(b * SUB, (b + 1) * SUB)
            lhs = jnp.concatenate(
                [ag[c, i, h, at] for i in range(NX) for h in range(heads)], axis=1
            )
            leave[c, at] = product(lhs, wg[1 - z], 1, 0).astype(BF16)
            sum_copy(c, b).start()
            part[c, at] = product(lhs, wg[z], 1, 0)

    def unit(u, carry):
        c, h = u // heads, lax.rem(u, heads)
        q = q_ref[h, c].astype(F32) * FACTOR
        q_high = q.astype(BF16)
        q2[:, :HEAD] = q_high
        q2[:, HEAD:] = (q - q_high.astype(F32)).astype(BF16)
        lanes = pl.ds(pl.multiple_of(h * HEAD, HEAD), HEAD)
        fold_chunk(
            q2, tk_ref[:, lanes], tv_ref[:, lanes], [None], m_ref, l_ref, acc_ref, s_ref, first=True
        )
        has_halo = jnp.where(c == 0, has_left.astype(jnp.int32), has_right.astype(jnp.int32))

        def visit(k, carry):
            @pl.when(k == 2)
            def _():
                pl.when(u == 0)(lambda: serve(0))
                pl.when(c == 0)(lambda: par_copy(h).wait_recv())

            @pl.when(k == 3)
            def _():
                @pl.when(u > 0)
                def _():
                    forward((u - 1) // heads, lax.rem(u - 1, heads))

                @pl.when(u == 1)
                def _():
                    for zc in range(2):
                        for step in (1, 3, 2):
                            w_copy(step, zc).wait_recv()
                            w_forward(step, zc).start()

            pl.when(k == 2 * n_rows + 1)(lambda: parcol_copy(h, c).wait_recv())
            pl.when(k == 2 * n_rows + 2)(lambda: zcol_copy(h, c).wait_recv())

            own = k < 2 * n_rows
            row_i = jnp.where(own, k // 2, k - 2 * n_rows)
            gap = jnp.where(own, lax.rem(k, 2), 1)
            row = jnp.where(row_i == 0, 1, jnp.where(row_i == 1, near, far))
            col = jnp.where(own, jnp.where(gap == 0, c + 1, 2 - c), 3 * c)
            away = (row_i > 0).astype(jnp.int32)
            pens = []
            for kt in range(2):
                pen = []
                for qt in range(2):
                    ok = (
                        (away <= radius[2 + qt, c])
                        & (gap <= radius[4 + qt, c])
                        & (abs(qt - kt) <= radius[qt, c])
                    )
                    pen.append(jnp.where(ok, 0.0, FAR))
                pens.append(jnp.where(late, pen[1], pen[0]))
            block = kvh.at[h, row, col]
            fold_chunk(q2, block[0], block[1], pens, m_ref, l_ref, acc_ref, s_ref)
            return carry

        lax.fori_loop(0, n_rows * (2 + has_halo), visit, 0)
        ag[c, x, h] = (acc_ref[...] / l_ref[...]).T.astype(BF16)
        for way in range(2):
            ag_copy(c, h, way).start()
        pl.when(u < heads - 1)(lambda: serve(u + 1))

        @pl.when(u == heads)
        def _():
            for zc in range(2):
                w_own(zc).wait()
                for step in (1, 3, 2):
                    w_forward(step, zc).wait_recv()

        @pl.when((u == heads) | (u == 2 * heads - 1))
        def _():
            pl.when(u > heads)(lambda: forward(1, heads - 1))
            project(c - (u == heads).astype(jnp.int32))

        return carry

    lax.fori_loop(0, 2 * heads, unit, 0)

    for c in range(2):
        for b in range(tokens // SUB):
            at = slice(b * SUB, (b + 1) * SUB)
            sum_copy(c, b).wait_recv()
            out_ref[c, at] = (part[c, at] + arrive[c, at].astype(F32)).astype(BF16)

    for c in range(2):
        for b in range(tokens // SUB):
            sum_copy(c, b).wait_send()
        for h in range(heads):
            ag_forward(c, h).wait_send()
            for way in range(2):
                ag_copy(c, h, way).wait_send()
    for zc in range(2):
        for step in range(1, NX):
            w_copy(step, zc).wait_send()
            w_forward(step, zc).wait_send()
    for h in range(heads):
        par_copy(h).wait_send()
        pl.when(inner)(lambda h=h: z_copy(h).wait_send())
        for side in range(2):
            when_side(side, lambda h=h, side=side: row_copy(h, side).wait_send())
            when_from(side, lambda h=h, side=side: parcol_copy(h, side).wait_send())

            @pl.when(inner & (has_right if side == 0 else has_left))
            def _():
                zcol_copy(h, side).wait_send()


def layer(radius, q, kv, text_keys, text_values, out_weight):
    heads, cols, tokens, _ = q.shape
    width = heads * HEAD
    dma = pltpu.SemaphoreType.DMA
    vmem = pl.BlockSpec(memory_space=pltpu.VMEM)
    blocks = tokens // SUB
    return pl.pallas_call(
        layer_kernel,
        in_specs=[
            pl.BlockSpec(memory_space=pltpu.SMEM),
            vmem, vmem, vmem, vmem,
            pl.BlockSpec(memory_space=pl.ANY),
        ],
        out_specs=vmem,
        out_shape=jax.ShapeDtypeStruct((cols, tokens, width), BF16),
        scratch_shapes=[
            pltpu.VMEM((heads, 3, 4, 2, tokens, HEAD), BF16),
            pltpu.VMEM((tokens, 2 * HEAD), BF16),
            pltpu.VMEM((1, tokens), F32),
            pltpu.VMEM((1, tokens), F32),
            pltpu.VMEM((HEAD, tokens), F32),
            pltpu.VMEM((blocks, tokens, SUB), F32),
            pltpu.VMEM((cols, NX, heads, tokens, HEAD), BF16),
            pltpu.VMEM((2, NX * width, width), BF16),
            pltpu.VMEM((cols, tokens, width), F32),
            pltpu.VMEM((cols, tokens, width), BF16),
            pltpu.VMEM((cols, tokens, width), BF16),
            dma((heads, 2)), dma((heads, 2)),
            dma((heads,)), dma((heads,)),
            dma((heads,)), dma((heads,)),
            dma((heads, 2)), dma((heads, 2)),
            dma((heads, 2)), dma((heads, 2)),
            dma((NX - 1, 2)), dma((NX - 1, 2)),
            dma((NX - 1, 2)), dma((NX - 1, 2)),
            dma((2,)),
            dma((cols, heads, 2)), dma((cols, heads, 2)),
            dma((cols, heads)), dma((cols, heads)),
            dma((cols, blocks)), dma((cols, blocks)),
        ],
        compiler_params=pltpu.CompilerParams(
            collective_id=0, has_side_effects=True, vmem_limit_bytes=60 * 1024 * 1024
        ),
        cost_estimate=pl.CostEstimate(
            flops=40_000_000_000, bytes_accessed=18_000_000, transcendentals=30_000_000
        ),
        name="layer",
    )(radius, q, kv, text_keys, text_values, out_weight)


def shards(queries, video_keys, video_values, text_keys, text_values, tile_radius, out_weight):
    n_frames, height, _, _ = queries.shape
    q = tiled(queries)
    kv = jnp.stack([tiled(video_keys), tiled(video_values)], axis=2)
    radius = tile_radius[:, :, 0, :].reshape(6, -1)
    return untiled(layer(radius, q, kv, text_keys, text_values, out_weight), n_frames, height)


def solution(mesh):
    placed = (
        P(None, "ha", "wa", "hd"),
        P(None, "ha", "wa", "hd"),
        P(None, "ha", "wa", "hd"),
        P(None, "hd"),
        P(None, "hd"),
        P(None, None, "ha", "wa"),
        P("hd", None),
    )
    return jax.shard_map(
        shards, mesh=mesh, in_specs=placed, out_specs=P(None, "ha", "wa", "hd"), check_vma=False
    )
```

```python
import functools

import jax
import jax.numpy as jnp
from jax import lax
from jax.experimental import pallas as pl
from jax.experimental.pallas import tpu as pltpu
from jax.sharding import PartitionSpec as P

HEAD = 128
TILE_W = 8
FACTOR = 1.4426950408889634 * HEAD ** (-0.5)
FAR = 1e30
LOG3 = 1.5849625007211562
TEXT_SLOT = 12
SUB = 256
NX = 4
BF16 = jnp.bfloat16
F32 = jnp.float32
MESH = pl.DeviceIdType.MESH


def tiled(block):
    frames, height, across, channels = block.shape
    cols = across // TILE_W
    heads = channels // HEAD
    cut = block.reshape(frames, height, cols, TILE_W, heads, HEAD)
    return cut.transpose(4, 2, 0, 1, 3, 5).reshape(heads, cols, -1, HEAD)


def untiled(tiles, frames, height):
    cols, _, channels = tiles.shape
    cut = tiles.reshape(cols, frames, height, TILE_W, channels)
    return cut.transpose(1, 2, 0, 3, 4).reshape(frames, height, cols * TILE_W, channels)


def product(a, b, over_a, over_b):
    return lax.dot_general(a, b, (((over_a,), (over_b,)), ((), ())), preferred_element_type=F32)


def score_part(q2, k, part, s_ref, top_ref):
    at = slice(part * SUB, (part + 1) * SUB)
    s = product(jnp.concatenate([k, k], axis=1), q2[at], 1, 1)
    s_ref[...] = s
    keys = k.shape[0] // 2
    for t in range(2):
        top_ref[t : t + 1, at] = jnp.max(s[t * keys : (t + 1) * keys], axis=0, keepdims=True)


def blend_part(v, pens, part, s_ref, top_ref, m_ref, l_ref, acc_ref):
    at = slice(part * SUB, (part + 1) * SUB)
    keys = v.shape[0] // 2
    rows = [pen[:, at] for pen in pens]
    m_old = m_ref[:, at]
    m_new = m_old
    for t in range(2):
        m_new = jnp.maximum(m_new, top_ref[t : t + 1, at] - rows[t])
    weights = [
        jnp.exp2(s_ref[t * keys : (t + 1) * keys] - (m_new + rows[t])) for t in range(2)
    ]
    total = sum(jnp.sum(weight, axis=0, keepdims=True) for weight in weights)
    low = jnp.concatenate([weight.astype(BF16) for weight in weights], axis=0)
    shrink = jnp.exp2(m_old - m_new)
    l_ref[:, at] = l_ref[:, at] * shrink + total
    acc_ref[:, at] = acc_ref[:, at] * shrink + product(v, low, 0, 0)
    m_ref[:, at] = m_new


def pair_at(p):
    unit = p // 2
    pair = lax.rem(p, 2)
    for start, count, first_unit, first_pair in (
        (8, 3, 0, 2), (14, 2, 4, 0), (18, 3, 2, 2), (24, 2, 4, 2), (28, 1, 4, 4),
    ):
        here = p >= start
        unit = jnp.where(here, first_unit + (p - start) // count, unit)
        pair = jnp.where(here, first_pair + lax.rem(p - start, count), pair)
    return unit, pair


STEPS = 30


def layer_kernel(
    radius, q_ref, kv_ref, tk_ref, tv_ref, w_ref, out_ref,
    kvh, q2, m_ref, l_ref, acc_ref, top0, top1, s00, s01, s02, s10, s11, s12,
    ag, wg, part, part_far, leave, arrive,
    row_s, row_r, par_s, par_r, z_s, z_r, parcol_s, parcol_r, zcol_s, zcol_r,
    w_s, w_r, wf_s, wf_r, wl, ag_s, ag_r, agf_s, agf_r, sum_s, sum_r,
):
    heads = q_ref.shape[0]
    tokens = q_ref.shape[2]
    width = heads * HEAD
    half = width // 2
    ha, wa, hd = lax.axis_index("ha"), lax.axis_index("wa"), lax.axis_index("hd")
    last = lax.axis_size("wa") - 1
    core = lax.rem(ha, 2)
    partner = ha + 1 - 2 * core
    inner = (ha == 1) | (ha == 2)
    peer = 3 - ha
    x = lax.rem(hd, NX)
    z = hd // NX
    near = 2 - 2 * core
    far = 2 * core
    has_left, has_right = wa > 0, wa < last

    def x_at(step):
        return z * NX + lax.rem(x + step, NX)

    def remote(src, dst, send, recv, device):
        return pltpu.make_async_remote_copy(
            src_ref=src, dst_ref=dst, send_sem=send, recv_sem=recv,
            device_id=device, device_id_type=MESH,
        )

    def row_copy(h, side):
        return remote(
            kv_ref.at[h, 1 - side], kvh.at[h, 4 + 3 * side], row_s.at[h, side], row_r.at[h, side],
            {"wa": wa + 1 - 2 * side},
        )

    def par_copy(h):
        return remote(
            kv_ref.at[h], kvh.at[h, pl.ds(4 * far + 1, 2)], par_s.at[h], par_r.at[h], {"ha": partner}
        )

    def z_copy(h):
        return remote(
            kv_ref.at[h], kvh.at[h, pl.ds(4 * near + 1, 2)], z_s.at[h], z_r.at[h], {"ha": peer}
        )

    def parcol_copy(h, side):
        return remote(
            kvh.at[h, 4 + 3 * side], kvh.at[h, 4 * far + 3 * side],
            parcol_s.at[h, side], parcol_r.at[h, side], {"ha": partner},
        )

    def zcol_copy(h, side):
        return remote(
            kvh.at[h, 4 * far + 2 - side], kvh.at[h, 4 * far + 3 * side],
            zcol_s.at[h, side], zcol_r.at[h, side], {"wa": wa + 1 - 2 * side},
        )

    def w_copy(step, zc):
        cols = pl.multiple_of((zc * NX + lax.rem(x + step, NX)) * width, HEAD)
        return remote(
            w_ref.at[pl.ds(core * half, half), pl.ds(cols, width)],
            wg.at[zc, pl.ds(x * width + core * half, half)],
            w_s.at[step - 1, zc], w_r.at[step - 1, zc], {"hd": x_at(step)},
        )

    def w_forward(step, zc):
        rows = pl.ds(lax.rem(x + NX - step, NX) * width + core * half, half)
        return remote(
            wg.at[zc, rows], wg.at[zc, rows],
            wf_s.at[step - 1, zc], wf_r.at[step - 1, zc], {"ha": partner},
        )

    def w_own(zc):
        cols = pl.multiple_of((zc * NX + x) * width, HEAD)
        return pltpu.make_async_copy(
            w_ref.at[:, pl.ds(cols, width)], wg.at[zc, pl.ds(x * width, width)], wl.at[zc]
        )

    def ag_copy(c, h, way):
        return remote(
            ag.at[c, x, h], ag.at[c, x, h], ag_s.at[c, h, way], ag_r.at[c, h, way],
            {"hd": x_at(1 + 2 * way)},
        )

    def ag_forward(c, h):
        block = ag.at[c, lax.rem(x + NX - 1 + 2 * c, NX), h]
        return remote(
            block, block, agf_s.at[c, h], agf_r.at[c, h], {"hd": x_at(1 + 2 * c)}
        )

    def sum_copy(c, b):
        at = pl.ds(b * SUB, SUB)
        return remote(
            leave.at[c, at], arrive.at[c, at], sum_s.at[c, b], sum_r.at[c, b],
            {"hd": lax.rem(hd + NX, 2 * NX)},
        )

    barrier = pltpu.get_barrier_semaphore()

    def greet(device):
        pl.semaphore_signal(barrier, inc=1, device_id=device, device_id_type=MESH)

    pl.when(has_left)(lambda: greet({"wa": wa - 1}))
    pl.when(has_right)(lambda: greet({"wa": wa + 1}))
    pl.when(inner)(lambda: greet({"ha": peer}))
    greet({"ha": partner})
    for step in range(1, NX):
        greet({"hd": x_at(step)})
    greet({"hd": lax.rem(hd + NX, 2 * NX)})
    pl.semaphore_wait(
        barrier,
        2 + NX - 1
        + has_left.astype(jnp.int32) + has_right.astype(jnp.int32) + inner.astype(jnp.int32),
    )

    def when_side(side, act):
        pl.when(has_right if side == 0 else has_left)(act)

    def when_from(side, act):
        pl.when(has_left if side == 0 else has_right)(act)

    def start_rows(h):
        for side in range(2):
            when_side(side, lambda side=side: row_copy(h, side).start())

    start_rows(0)
    for h in range(heads):
        pl.when(inner)(lambda h=h: z_copy(h).start())
        par_copy(h).start()
    for zc in range(2):
        w_own(zc).start()
        for step in (1, 3, 2):
            w_copy(step, zc).start()
    for h in range(heads):
        kvh[h, 5:7] = kv_ref[h]
        lanes = slice(h * HEAD, (h + 1) * HEAD)
        for copy in range(3):
            rows = slice(copy * SUB, (copy + 1) * SUB)
            kvh[h, TEXT_SLOT, 0, rows] = tk_ref[:, lanes]
            kvh[h, TEXT_SLOT, 1, rows] = tv_ref[:, lanes]
    for u in range(2 * heads):
        q = q_ref[u // 2, u % 2].astype(F32) * FACTOR
        q_high = q.astype(BF16)
        q2[u, :, :HEAD] = q_high
        q2[u, :, HEAD:] = (q - q_high.astype(F32)).astype(BF16)
    m_ref[...] = jnp.full_like(m_ref, -FAR)
    l_ref[...] = jnp.zeros_like(l_ref)
    acc_ref[...] = jnp.zeros_like(acc_ref)

    def serve(h):
        for side in range(2):
            when_from(side, lambda side=side: row_copy(h, side).wait_recv())
        pl.when(inner)(lambda: z_copy(h).wait_recv())
        for side in range(2):
            when_from(side, lambda side=side: parcol_copy(h, side).start())
        for side in range(2):

            @pl.when(inner & (has_right if side == 0 else has_left))
            def _():
                zcol_copy(h, side).start()

        pl.when(h < heads - 1)(lambda: start_rows(h + 1))

    late = lax.broadcasted_iota(jnp.int32, (1, tokens), 1) >= tokens // 2
    sets = ((s00, s01, s02), (s10, s11, s12))
    peaks = (top0, top1)
    parts = tokens // SUB

    def halo_at(c):
        return jnp.where(c == 0, has_left.astype(jnp.int32), has_right.astype(jnp.int32))

    def chunk_at(c, chunk):
        v = chunk - 1
        side_col = v >= 6
        row_i = jnp.where(side_col, v - 6, v // 2)
        gap = jnp.where(side_col, 1, lax.rem(v, 2))
        there = ((row_i < 2) | inner) & ((v < 6) | (halo_at(c) > 0))
        row = jnp.where(row_i == 0, 1, jnp.where(row_i == 1, near, far))
        col = jnp.where(side_col, 3 * c, jnp.where(gap == 0, c + 1, 2 - c))
        slot = jnp.where(there, 4 * row + col, 5 + c)
        slot = jnp.where(chunk == 0, TEXT_SLOT, slot)
        return slot, there, (row_i > 0).astype(jnp.int32), gap

    def score_step(u, pair, which, part_i):
        slot, _, _, _ = chunk_at(lax.rem(u, 2), 2 * pair + which)
        score_part(q2.at[u], kvh[u // 2, slot, 0], part_i, sets[which][part_i], peaks[which])

    def pens_of(u, pair, which):
        c = lax.rem(u, 2)
        chunk = 2 * pair + which
        _, there, away, gap = chunk_at(c, chunk)
        pens = []
        for kt in range(2):
            pen = []
            for qt in range(2):
                ok = (
                    there
                    & (away <= radius[2 + qt, c])
                    & (gap <= radius[4 + qt, c])
                    & (abs(qt - kt) <= radius[qt, c])
                )
                pen.append(jnp.where(chunk == 0, LOG3, jnp.where(ok, 0.0, FAR)))
            pens.append(jnp.where(late, pen[1], pen[0]))
        return pens

    def forward(u):
        h, c = u // 2, lax.rem(u, 2)
        ag_copy(c, h, c).wait_recv()
        ag_forward(c, h).start()

    def gathered(c, h):
        ag_copy(c, h, 1 - c).wait_recv()
        ag_forward(c, h).wait_recv()

    def rows_of(zc, h):
        return [wg[zc, i * width + h * HEAD : i * width + (h + 1) * HEAD] for i in range(NX)]

    def last_rows(zc):
        return jnp.concatenate(rows_of(zc, heads - 1), axis=0)

    def project_first(c):
        for h in range(heads - 1):
            gathered(c, h)
        for b in range(parts):
            at = slice(b * SUB, (b + 1) * SUB)
            lhs = jnp.concatenate(
                [ag[c, i, h, at] for h in range(heads - 1) for i in range(NX)], axis=1
            )
            for zc, out in ((1 - z, part_far), (z, part)):
                rhs = [block for h in range(heads - 1) for block in rows_of(zc, h)]
                out[c, at] = product(lhs, jnp.concatenate(rhs, axis=0), 1, 0)

    def project_last(c):
        h = heads - 1
        gathered(c, h)
        for b in range(parts):
            at = slice(b * SUB, (b + 1) * SUB)
            lhs = jnp.concatenate([ag[c, i, h, at] for i in range(NX)], axis=1)
            leave[c, at] = (part_far[c, at] + product(lhs, last_rows(1 - z), 1, 0)).astype(BF16)
            sum_copy(c, b).start()
        for b in range(parts):
            at = slice(b * SUB, (b + 1) * SUB)
            lhs = jnp.concatenate([ag[c, i, h, at] for i in range(NX)], axis=1)
            part[c, at] = part[c, at] + product(lhs, last_rows(z), 1, 0)

    for which in range(2):
        for part_i in range(parts):
            score_step(0, 0, which, part_i)

    def step(p, carry):
        u, pair = pair_at(p)
        u_next, pair_next = pair_at(jnp.minimum(p + 1, STEPS - 1))
        h_next, c_next = u_next // 2, lax.rem(u_next, 2)
        pl.when((pair_next == 1) & (c_next == 0))(lambda: par_copy(h_next).wait_recv())
        for at_step, h in ((6, 0), (16, 1), (23, 2)):
            pl.when(p == at_step)(lambda h=h: serve(h))

        @pl.when((pair_next == 4) & (p < STEPS - 1) & (halo_at(c_next) > 0))
        def _():
            parcol_copy(h_next, c_next).wait_recv()
            pl.when(inner)(lambda: zcol_copy(h_next, c_next).wait_recv())

        @pl.when(p == 17)
        def _():
            for zc in range(2):
                for hop in (1, 3, 2):
                    w_copy(hop, zc).wait_recv()
                    w_forward(hop, zc).start()

        for at_step, done in ((16, 0), (19, 1), (26, 2), (29, 3)):
            pl.when(p == at_step)(lambda done=done: forward(jnp.int32(done)))

        pens = [pens_of(u, pair, which) for which in range(2)]
        c, h = lax.rem(u, 2), u // 2
        for which in range(2):
            slot, _, _, _ = chunk_at(c, 2 * pair + which)
            for part_i in range(parts):
                blend_part(
                    kvh[h, slot, 1], pens[which], part_i, sets[which][part_i], peaks[which],
                    m_ref.at[u], l_ref.at[u], acc_ref.at[u],
                )
                score_step(u_next, pair_next, which, part_i)

        @pl.when(pair == 4)
        def _():
            ag[c, x, h] = (acc_ref[u] / l_ref[u]).T.astype(BF16)
            for way in range(2):
                ag_copy(c, h, way).start()

        return carry

    lax.fori_loop(0, STEPS, step, 0)

    for zc in range(2):
        w_own(zc).wait()
        for hop in (1, 3, 2):
            w_forward(hop, zc).wait_recv()
    project_first(0)
    forward(jnp.int32(4))
    project_first(1)
    forward(jnp.int32(5))
    project_last(0)
    project_last(1)

    for c in range(2):
        for b in range(tokens // SUB):
            at = slice(b * SUB, (b + 1) * SUB)
            sum_copy(c, b).wait_recv()
            out_ref[c, at] = (part[c, at] + arrive[c, at].astype(F32)).astype(BF16)

    for c in range(2):
        for b in range(tokens // SUB):
            sum_copy(c, b).wait_send()
        for h in range(heads):
            ag_forward(c, h).wait_send()
            for way in range(2):
                ag_copy(c, h, way).wait_send()
    for zc in range(2):
        for step in range(1, NX):
            w_copy(step, zc).wait_send()
            w_forward(step, zc).wait_send()
    for h in range(heads):
        par_copy(h).wait_send()
        pl.when(inner)(lambda h=h: z_copy(h).wait_send())
        for side in range(2):
            when_side(side, lambda h=h, side=side: row_copy(h, side).wait_send())
            when_from(side, lambda h=h, side=side: parcol_copy(h, side).wait_send())

            @pl.when(inner & (has_right if side == 0 else has_left))
            def _():
                zcol_copy(h, side).wait_send()


def layer(radius, q, kv, text_keys, text_values, out_weight):
    heads, cols, tokens, _ = q.shape
    width = heads * HEAD
    dma = pltpu.SemaphoreType.DMA
    vmem = pl.BlockSpec(memory_space=pltpu.VMEM)
    blocks = tokens // SUB
    return pl.pallas_call(
        layer_kernel,
        in_specs=[
            pl.BlockSpec(memory_space=pltpu.SMEM),
            vmem, vmem, vmem, vmem,
            pl.BlockSpec(memory_space=pl.ANY),
        ],
        out_specs=vmem,
        out_shape=jax.ShapeDtypeStruct((cols, tokens, width), BF16),
        scratch_shapes=[
            pltpu.VMEM((heads, TEXT_SLOT + 1, 2, tokens, HEAD), BF16),
            pltpu.VMEM((2 * heads, tokens, 2 * HEAD), BF16),
            pltpu.VMEM((2 * heads, 1, tokens), F32),
            pltpu.VMEM((2 * heads, 1, tokens), F32),
            pltpu.VMEM((2 * heads, HEAD, tokens), F32),
            pltpu.VMEM((2, tokens), F32),
            pltpu.VMEM((2, tokens), F32),
            *[pltpu.VMEM((tokens, SUB), F32)] * (2 * blocks),
            pltpu.VMEM((cols, NX, heads, tokens, HEAD), BF16),
            pltpu.VMEM((2, NX * width, width), BF16),
            pltpu.VMEM((cols, tokens, width), F32),
            pltpu.VMEM((cols, tokens, width), F32),
            pltpu.VMEM((cols, tokens, width), BF16),
            pltpu.VMEM((cols, tokens, width), BF16),
            dma((heads, 2)), dma((heads, 2)),
            dma((heads,)), dma((heads,)),
            dma((heads,)), dma((heads,)),
            dma((heads, 2)), dma((heads, 2)),
            dma((heads, 2)), dma((heads, 2)),
            dma((NX - 1, 2)), dma((NX - 1, 2)),
            dma((NX - 1, 2)), dma((NX - 1, 2)),
            dma((2,)),
            dma((cols, heads, 2)), dma((cols, heads, 2)),
            dma((cols, heads)), dma((cols, heads)),
            dma((cols, blocks)), dma((cols, blocks)),
        ],
        compiler_params=pltpu.CompilerParams(
            collective_id=0, has_side_effects=True, vmem_limit_bytes=60 * 1024 * 1024
        ),
        cost_estimate=pl.CostEstimate(
            flops=40_000_000_000, bytes_accessed=18_000_000, transcendentals=30_000_000
        ),
        name="layer",
    )(radius, q, kv, text_keys, text_values, out_weight)


def shards(queries, video_keys, video_values, text_keys, text_values, tile_radius, out_weight):
    n_frames, height, _, _ = queries.shape
    q = tiled(queries)
    kv = jnp.stack([tiled(video_keys), tiled(video_values)], axis=2)
    radius = tile_radius[:, :, 0, :].reshape(6, -1)
    return untiled(layer(radius, q, kv, text_keys, text_values, out_weight), n_frames, height)


def solution(mesh):
    placed = (
        P(None, "ha", "wa", "hd"),
        P(None, "ha", "wa", "hd"),
        P(None, "ha", "wa", "hd"),
        P(None, "hd"),
        P(None, "hd"),
        P(None, None, "ha", "wa"),
        P("hd", None),
    )
    return jax.shard_map(
        shards, mesh=mesh, in_specs=placed, out_specs=P(None, "ha", "wa", "hd"), check_vma=False
    )
```

```python
import functools

import jax
import jax.numpy as jnp
from jax import lax
from jax.experimental import pallas as pl
from jax.experimental.pallas import tpu as pltpu
from jax.sharding import PartitionSpec as P

HEAD = 128
TILE_W = 8
FACTOR = 1.4426950408889634 * HEAD ** (-0.5)
FAR = 1e30
LOG3 = 1.5849625007211562
TEXT_SLOT = 12
SUB = 256
NX = 4
BF16 = jnp.bfloat16
F32 = jnp.float32
MESH = pl.DeviceIdType.MESH


def tiled(block):
    frames, height, across, channels = block.shape
    cols = across // TILE_W
    heads = channels // HEAD
    cut = block.reshape(frames, height, cols, TILE_W, heads, HEAD)
    return cut.transpose(4, 2, 0, 1, 3, 5).reshape(heads, cols, -1, HEAD)


def untiled(tiles, frames, height):
    cols, _, channels = tiles.shape
    cut = tiles.reshape(cols, frames, height, TILE_W, channels)
    return cut.transpose(1, 2, 0, 3, 4).reshape(frames, height, cols * TILE_W, channels)


def product(a, b, over_a, over_b):
    return lax.dot_general(a, b, (((over_a,), (over_b,)), ((), ())), preferred_element_type=F32)


def score_part(q2, k, part, s_ref, top_ref):
    at = slice(part * SUB, (part + 1) * SUB)
    s = product(jnp.concatenate([k, k], axis=1), q2[at], 1, 1)
    s_ref[...] = s
    keys = k.shape[0] // 2
    for t in range(2):
        top_ref[t : t + 1, at] = jnp.max(s[t * keys : (t + 1) * keys], axis=0, keepdims=True)


def blend_part(v, pens, part, s_ref, top_ref, m_ref, l_ref, acc_ref):
    at = slice(part * SUB, (part + 1) * SUB)
    keys = v.shape[0] // 2
    rows = [pen[:, at] for pen in pens]
    m_old = m_ref[:, at]
    m_new = m_old
    for t in range(2):
        m_new = jnp.maximum(m_new, top_ref[t : t + 1, at] - rows[t])
    weights = [
        jnp.exp2(s_ref[t * keys : (t + 1) * keys] - (m_new + rows[t])) for t in range(2)
    ]
    total = sum(jnp.sum(weight, axis=0, keepdims=True) for weight in weights)
    low = jnp.concatenate([weight.astype(BF16) for weight in weights], axis=0)
    shrink = jnp.exp2(m_old - m_new)
    l_ref[:, at] = l_ref[:, at] * shrink + total
    acc_ref[:, at] = acc_ref[:, at] * shrink + product(v, low, 0, 0)
    m_ref[:, at] = m_new


ORDER = (
    (0, 0, 2), (1, 0, 2), (0, 2, 2), (1, 2, 2), (2, 0, 2), (0, 4, 1), (1, 4, 1), (2, 2, 1),
    (3, 0, 2), (2, 3, 1), (3, 2, 2), (2, 4, 1), (3, 4, 1), (4, 0, 5), (5, 0, 5),
)


def pair_at(p):
    unit, pair, start = jnp.int32(0), p, 0
    for run_unit, first, count in ORDER:
        if start > 0:
            here = p >= start
            unit = jnp.where(here, run_unit, unit)
            pair = jnp.where(here, p + (first - start), pair)
        start += count
    return unit, pair


STEPS = 30


def layer_kernel(
    radius, q_ref, kv_ref, tk_ref, tv_ref, w_ref, out_ref,
    kvh, q2, m_ref, l_ref, acc_ref, top0, top1, s00, s01, s02, s10, s11, s12,
    ag, wg, part, part_far, leave, arrive,
    row_s, row_r, par_s, par_r, z_s, z_r, parcol_s, parcol_r, zcol_s, zcol_r,
    w_s, w_r, wf_s, wf_r, wl, ag_s, ag_r, agf_s, agf_r, end_s, end_r, sum_s, sum_r,
):
    heads = q_ref.shape[0]
    tokens = q_ref.shape[2]
    width = heads * HEAD
    half = width // 2
    ha, wa, hd = lax.axis_index("ha"), lax.axis_index("wa"), lax.axis_index("hd")
    last = lax.axis_size("wa") - 1
    core = lax.rem(ha, 2)
    partner = ha + 1 - 2 * core
    inner = (ha == 1) | (ha == 2)
    peer = 3 - ha
    x = lax.rem(hd, NX)
    z = hd // NX
    near = 2 - 2 * core
    far = 2 * core
    has_left, has_right = wa > 0, wa < last

    def x_at(step):
        return z * NX + lax.rem(x + step, NX)

    def remote(src, dst, send, recv, device):
        return pltpu.make_async_remote_copy(
            src_ref=src, dst_ref=dst, send_sem=send, recv_sem=recv,
            device_id=device, device_id_type=MESH,
        )

    def row_copy(h, side):
        return remote(
            kv_ref.at[h, 1 - side], kvh.at[h, 4 + 3 * side], row_s.at[h, side], row_r.at[h, side],
            {"wa": wa + 1 - 2 * side},
        )

    def par_copy(h):
        return remote(
            kv_ref.at[h], kvh.at[h, pl.ds(4 * far + 1, 2)], par_s.at[h], par_r.at[h], {"ha": partner}
        )

    def z_copy(h):
        return remote(
            kv_ref.at[h], kvh.at[h, pl.ds(4 * near + 1, 2)], z_s.at[h], z_r.at[h], {"ha": peer}
        )

    def parcol_copy(h, side):
        return remote(
            kvh.at[h, 4 + 3 * side], kvh.at[h, 4 * far + 3 * side],
            parcol_s.at[h, side], parcol_r.at[h, side], {"ha": partner},
        )

    def zcol_copy(h, side):
        return remote(
            kvh.at[h, 4 * far + 2 - side], kvh.at[h, 4 * far + 3 * side],
            zcol_s.at[h, side], zcol_r.at[h, side], {"wa": wa + 1 - 2 * side},
        )

    def w_copy(step, zc):
        cols = pl.multiple_of((zc * NX + lax.rem(x + step, NX)) * width, HEAD)
        return remote(
            w_ref.at[pl.ds(core * half, half), pl.ds(cols, width)],
            wg.at[zc, pl.ds(x * width + core * half, half)],
            w_s.at[step - 1, zc], w_r.at[step - 1, zc], {"hd": x_at(step)},
        )

    def w_forward(step, zc):
        rows = pl.ds(lax.rem(x + NX - step, NX) * width + core * half, half)
        return remote(
            wg.at[zc, rows], wg.at[zc, rows],
            wf_s.at[step - 1, zc], wf_r.at[step - 1, zc], {"ha": partner},
        )

    def w_own(zc):
        cols = pl.multiple_of((zc * NX + x) * width, HEAD)
        return pltpu.make_async_copy(
            w_ref.at[:, pl.ds(cols, width)], wg.at[zc, pl.ds(x * width, width)], wl.at[zc]
        )

    def ag_copy(c, h, way):
        return remote(
            ag.at[c, x, h], ag.at[c, x, h], ag_s.at[c, h, way], ag_r.at[c, h, way],
            {"hd": x_at(1 + 2 * way)},
        )

    def ag_forward(c, h):
        block = ag.at[c, lax.rem(x + NX - 1 + 2 * c, NX), h]
        return remote(
            block, block, agf_s.at[c, h], agf_r.at[c, h], {"hd": x_at(1 + 2 * c)}
        )

    def end_copy(c, b, hop):
        block = ag.at[c, x, heads - 1, pl.ds(b * SUB, SUB)]
        return remote(
            block, block, end_s.at[c, b, hop - 1], end_r.at[c, b, hop - 1], {"hd": x_at(hop)}
        )

    def sum_copy(c, b):
        at = pl.ds(b * SUB, SUB)
        return remote(
            leave.at[c, at], arrive.at[c, at], sum_s.at[c, b], sum_r.at[c, b],
            {"hd": lax.rem(hd + NX, 2 * NX)},
        )

    barrier = pltpu.get_barrier_semaphore()

    def greet(device):
        pl.semaphore_signal(barrier, inc=1, device_id=device, device_id_type=MESH)

    pl.when(has_left)(lambda: greet({"wa": wa - 1}))
    pl.when(has_right)(lambda: greet({"wa": wa + 1}))
    pl.when(inner)(lambda: greet({"ha": peer}))
    greet({"ha": partner})
    for step in range(1, NX):
        greet({"hd": x_at(step)})
    greet({"hd": lax.rem(hd + NX, 2 * NX)})
    pl.semaphore_wait(
        barrier,
        2 + NX - 1
        + has_left.astype(jnp.int32) + has_right.astype(jnp.int32) + inner.astype(jnp.int32),
    )

    def when_side(side, act):
        pl.when(has_right if side == 0 else has_left)(act)

    def when_from(side, act):
        pl.when(has_left if side == 0 else has_right)(act)

    def start_rows(h):
        for side in range(2):
            when_side(side, lambda side=side: row_copy(h, side).start())

    start_rows(0)
    for h in range(heads):
        pl.when(inner)(lambda h=h: z_copy(h).start())
        par_copy(h).start()
    for zc in range(2):
        w_own(zc).start()
        for step in (1, 3, 2):
            w_copy(step, zc).start()
    for h in range(heads):
        kvh[h, 5:7] = kv_ref[h]
        lanes = slice(h * HEAD, (h + 1) * HEAD)
        for copy in range(3):
            rows = slice(copy * SUB, (copy + 1) * SUB)
            kvh[h, TEXT_SLOT, 0, rows] = tk_ref[:, lanes]
            kvh[h, TEXT_SLOT, 1, rows] = tv_ref[:, lanes]
    for u in range(2 * heads):
        q = q_ref[u // 2, u % 2].astype(F32) * FACTOR
        q_high = q.astype(BF16)
        q2[u, :, :HEAD] = q_high
        q2[u, :, HEAD:] = (q - q_high.astype(F32)).astype(BF16)
    m_ref[...] = jnp.full_like(m_ref, -FAR)
    l_ref[...] = jnp.zeros_like(l_ref)
    acc_ref[...] = jnp.zeros_like(acc_ref)

    def serve_z(h):
        z_copy(h).wait_recv()
        for side in range(2):
            when_side(side, lambda side=side: zcol_copy(h, side).start())
        if h < heads - 1:
            start_rows(h + 1)

    def serve_rows(h):
        for side in range(2):

            @pl.when(has_left if side == 0 else has_right)
            def _(side=side):
                row_copy(h, side).wait_recv()
                parcol_copy(h, side).start()

    late = lax.broadcasted_iota(jnp.int32, (1, tokens), 1) >= tokens // 2
    sets = ((s00, s01, s02), (s10, s11, s12))
    peaks = (top0, top1)
    parts = tokens // SUB

    def halo_at(c):
        return jnp.where(c == 0, has_left.astype(jnp.int32), has_right.astype(jnp.int32))

    def chunk_at(c, chunk):
        v = chunk - 1
        side_col = v >= 6
        row_i = jnp.where(side_col, v - 6, v // 2)
        gap = jnp.where(side_col, 1, lax.rem(v, 2))
        there = ((row_i < 2) | inner) & ((v < 6) | (halo_at(c) > 0))
        row = jnp.where(row_i == 0, 1, jnp.where(row_i == 1, near, far))
        col = jnp.where(side_col, 3 * c, jnp.where(gap == 0, c + 1, 2 - c))
        slot = jnp.where(there, 4 * row + col, 5 + c)
        slot = jnp.where(chunk == 0, TEXT_SLOT, slot)
        return slot, there, (row_i > 0).astype(jnp.int32), gap

    def score_step(u, pair, which, part_i):
        slot, _, _, _ = chunk_at(lax.rem(u, 2), 2 * pair + which)
        score_part(q2.at[u], kvh[u // 2, slot, 0], part_i, sets[which][part_i], peaks[which])

    def pens_of(u, pair, which):
        c = lax.rem(u, 2)
        chunk = 2 * pair + which
        _, there, away, gap = chunk_at(c, chunk)
        pens = []
        for kt in range(2):
            pen = []
            for qt in range(2):
                ok = (
                    there
                    & (away <= radius[2 + qt, c])
                    & (gap <= radius[4 + qt, c])
                    & (abs(qt - kt) <= radius[qt, c])
                )
                pen.append(jnp.where(chunk == 0, LOG3, jnp.where(ok, 0.0, FAR)))
            pens.append(jnp.where(late, pen[1], pen[0]))
        return pens

    def forward(u):
        h, c = u // 2, lax.rem(u, 2)
        ag_copy(c, h, c).wait_recv()
        ag_forward(c, h).start()

    def rows_of(zc, h):
        return [wg[zc, i * width + h * HEAD : i * width + (h + 1) * HEAD] for i in range(NX)]

    def last_rows(zc):
        return jnp.concatenate(rows_of(zc, heads - 1), axis=0)

    def project_first(c):
        for h in range(heads - 1):
            ag_copy(c, h, 1 - c).wait_recv()
            ag_forward(c, h).wait_recv()
        for b in range(parts):
            at = slice(b * SUB, (b + 1) * SUB)
            lhs = jnp.concatenate(
                [ag[c, i, h, at] for h in range(heads - 1) for i in range(NX)], axis=1
            )
            for zc, out in ((1 - z, part_far), (z, part)):
                rhs = [block for h in range(heads - 1) for block in rows_of(zc, h)]
                out[c, at] = product(lhs, jnp.concatenate(rhs, axis=0), 1, 0)

    def project_last(c, b):
        for hop in (1, 3, 2):
            end_copy(c, b, hop).wait_recv()
        at = slice(b * SUB, (b + 1) * SUB)
        lhs = jnp.concatenate([ag[c, i, heads - 1, at] for i in range(NX)], axis=1)
        leave[c, at] = (part_far[c, at] + product(lhs, last_rows(1 - z), 1, 0)).astype(BF16)
        sum_copy(c, b).start()
        part[c, at] = part[c, at] + product(lhs, last_rows(z), 1, 0)

    for which in range(2):
        for part_i in range(parts):
            score_step(0, 0, which, part_i)

    def step(p, carry):
        u, pair = carry
        u_next, pair_next = pair_at(jnp.minimum(p + 1, STEPS - 1))
        h_next, c_next = u_next // 2, lax.rem(u_next, 2)
        pl.when((pair_next == 1) & (c_next == 0))(lambda: par_copy(h_next).wait_recv())
        for at_step, h in ((3, 0), (9, 1), (14, 2)):
            pl.when((p == at_step) & inner)(lambda h=h: serve_z(h))
        for at_step, h in ((5, 1), (11, 2)):
            pl.when((p == at_step) & ~inner)(lambda h=h: start_rows(h))
        for at_step, h in ((4, 0), (14, 1), (21, 2)):
            pl.when(p == at_step)(lambda h=h: serve_rows(h))

        @pl.when((pair_next == 4) & (p < STEPS - 1) & (halo_at(c_next) > 0))
        def _():
            parcol_copy(h_next, c_next).wait_recv()
            pl.when(inner)(lambda: zcol_copy(h_next, c_next).wait_recv())

        @pl.when(p == 15)
        def _():
            for zc in range(2):
                for hop in (1, 3, 2):
                    w_copy(hop, zc).wait_recv()
                    w_forward(hop, zc).start()

        for at_step, done in ((17, 0), (20, 1), (24, 2), (27, 3)):
            pl.when(p == at_step)(lambda done=done: forward(jnp.int32(done)))

        @pl.when(p == STEPS - 2)
        def _():
            for zc in range(2):
                w_own(zc).wait()
                for hop in (1, 3, 2):
                    w_forward(hop, zc).wait_recv()
            project_first(0)

        pl.when(p == STEPS - 1)(lambda: project_last(0, 0))

        pens = [pens_of(u, pair, which) for which in range(2)]
        c, h = lax.rem(u, 2), u // 2
        for which in range(2):
            slot, _, _, _ = chunk_at(c, 2 * pair + which)
            for part_i in range(parts):
                blend_part(
                    kvh[h, slot, 1], pens[which], part_i, sets[which][part_i], peaks[which],
                    m_ref.at[u], l_ref.at[u], acc_ref.at[u],
                )
                score_step(u_next, pair_next, which, part_i)

        @pl.when((pair == 4) & (h < heads - 1))
        def _():
            ag[c, x, h] = (acc_ref[u] / l_ref[u]).T.astype(BF16)
            for way in range(2):
                ag_copy(c, h, way).start()

        @pl.when((pair == 4) & (h == heads - 1))
        def _():
            for b in range(parts):
                at = slice(b * SUB, (b + 1) * SUB)
                ag[c, x, heads - 1, at] = (acc_ref[u, :, at] / l_ref[u, :, at]).T.astype(BF16)
                for hop in (1, 3, 2):
                    end_copy(c, b, hop).start()

        return u_next, pair_next

    lax.fori_loop(0, STEPS, step, (jnp.int32(0), jnp.int32(0)))

    project_last(0, 1)
    project_first(1)
    project_last(0, 2)
    for b in range(parts):
        project_last(1, b)

    for c in range(2):
        for b in range(tokens // SUB):
            at = slice(b * SUB, (b + 1) * SUB)
            sum_copy(c, b).wait_recv()
            out_ref[c, at] = (part[c, at] + arrive[c, at].astype(F32)).astype(BF16)

    for c in range(2):
        for b in range(tokens // SUB):
            sum_copy(c, b).wait_send()
            for hop in range(1, NX):
                end_copy(c, b, hop).wait_send()
        for h in range(heads - 1):
            ag_forward(c, h).wait_send()
            for way in range(2):
                ag_copy(c, h, way).wait_send()
    for zc in range(2):
        for step in range(1, NX):
            w_copy(step, zc).wait_send()
            w_forward(step, zc).wait_send()
    for h in range(heads):
        par_copy(h).wait_send()
        pl.when(inner)(lambda h=h: z_copy(h).wait_send())
        for side in range(2):
            when_side(side, lambda h=h, side=side: row_copy(h, side).wait_send())
            when_from(side, lambda h=h, side=side: parcol_copy(h, side).wait_send())

            @pl.when(inner & (has_right if side == 0 else has_left))
            def _():
                zcol_copy(h, side).wait_send()


def layer(radius, q, kv, text_keys, text_values, out_weight):
    heads, cols, tokens, _ = q.shape
    width = heads * HEAD
    dma = pltpu.SemaphoreType.DMA
    vmem = pl.BlockSpec(memory_space=pltpu.VMEM)
    blocks = tokens // SUB
    return pl.pallas_call(
        layer_kernel,
        in_specs=[
            pl.BlockSpec(memory_space=pltpu.SMEM),
            vmem, vmem, vmem, vmem,
            pl.BlockSpec(memory_space=pl.ANY),
        ],
        out_specs=vmem,
        out_shape=jax.ShapeDtypeStruct((cols, tokens, width), BF16),
        scratch_shapes=[
            pltpu.VMEM((heads, TEXT_SLOT + 1, 2, tokens, HEAD), BF16),
            pltpu.VMEM((2 * heads, tokens, 2 * HEAD), BF16),
            pltpu.VMEM((2 * heads, 1, tokens), F32),
            pltpu.VMEM((2 * heads, 1, tokens), F32),
            pltpu.VMEM((2 * heads, HEAD, tokens), F32),
            pltpu.VMEM((2, tokens), F32),
            pltpu.VMEM((2, tokens), F32),
            *[pltpu.VMEM((tokens, SUB), F32)] * (2 * blocks),
            pltpu.VMEM((cols, NX, heads, tokens, HEAD), BF16),
            pltpu.VMEM((2, NX * width, width), BF16),
            pltpu.VMEM((cols, tokens, width), F32),
            pltpu.VMEM((cols, tokens, width), F32),
            pltpu.VMEM((cols, tokens, width), BF16),
            pltpu.VMEM((cols, tokens, width), BF16),
            dma((heads, 2)), dma((heads, 2)),
            dma((heads,)), dma((heads,)),
            dma((heads,)), dma((heads,)),
            dma((heads, 2)), dma((heads, 2)),
            dma((heads, 2)), dma((heads, 2)),
            dma((NX - 1, 2)), dma((NX - 1, 2)),
            dma((NX - 1, 2)), dma((NX - 1, 2)),
            dma((2,)),
            dma((cols, heads - 1, 2)), dma((cols, heads - 1, 2)),
            dma((cols, heads - 1)), dma((cols, heads - 1)),
            dma((cols, blocks, NX - 1)), dma((cols, blocks, NX - 1)),
            dma((cols, blocks)), dma((cols, blocks)),
        ],
        compiler_params=pltpu.CompilerParams(
            collective_id=0, has_side_effects=True, vmem_limit_bytes=60 * 1024 * 1024
        ),
        cost_estimate=pl.CostEstimate(
            flops=40_000_000_000, bytes_accessed=18_000_000, transcendentals=30_000_000
        ),
        name="layer",
    )(radius, q, kv, text_keys, text_values, out_weight)


def shards(queries, video_keys, video_values, text_keys, text_values, tile_radius, out_weight):
    n_frames, height, _, _ = queries.shape
    q = tiled(queries)
    kv = jnp.stack([tiled(video_keys), tiled(video_values)], axis=2)
    radius = tile_radius[:, :, 0, :].reshape(6, -1)
    return untiled(layer(radius, q, kv, text_keys, text_values, out_weight), n_frames, height)


def solution(mesh):
    placed = (
        P(None, "ha", "wa", "hd"),
        P(None, "ha", "wa", "hd"),
        P(None, "ha", "wa", "hd"),
        P(None, "hd"),
        P(None, "hd"),
        P(None, None, "ha", "wa"),
        P("hd", None),
    )
    return jax.shard_map(
        shards, mesh=mesh, in_specs=placed, out_specs=P(None, "ha", "wa", "hd"), check_vma=False
    )
```

```python
import functools

import jax
import jax.numpy as jnp
from jax import lax
from jax.experimental import pallas as pl
from jax.experimental.pallas import tpu as pltpu
from jax.sharding import PartitionSpec as P

HEAD = 128
TILE_W = 8
FACTOR = 1.4426950408889634 * HEAD ** (-0.5)
FAR = 1e30
LOG3 = 1.5849625007211562
TEXT_SLOT = 12
SUB = 256
NX = 4
BF16 = jnp.bfloat16
F32 = jnp.float32
MESH = pl.DeviceIdType.MESH


def tiled(block):
    frames, height, across, channels = block.shape
    cols = across // TILE_W
    heads = channels // HEAD
    cut = block.reshape(frames, height, cols, TILE_W, heads, HEAD)
    return cut.transpose(4, 2, 0, 1, 3, 5).reshape(heads, cols, -1, HEAD)


def untiled(tiles, frames, height):
    cols, _, channels = tiles.shape
    cut = tiles.reshape(cols, frames, height, TILE_W, channels)
    return cut.transpose(1, 2, 0, 3, 4).reshape(frames, height, cols * TILE_W, channels)


def product(a, b, over_a, over_b):
    return lax.dot_general(a, b, (((over_a,), (over_b,)), ((), ())), preferred_element_type=F32)


def score_part(q2, k, part, s_ref, top_ref):
    at = slice(part * SUB, (part + 1) * SUB)
    s = product(jnp.concatenate([k, k], axis=1), q2[at], 1, 1)
    s_ref[...] = s
    keys = k.shape[0] // 2
    for t in range(2):
        top_ref[t : t + 1, at] = jnp.max(s[t * keys : (t + 1) * keys], axis=0, keepdims=True)


def blend_part(v, pens, part, s_ref, top_ref, m_ref, l_ref, acc_ref):
    at = slice(part * SUB, (part + 1) * SUB)
    keys = v.shape[0] // 2
    rows = [pen[:, at] for pen in pens]
    m_old = m_ref[:, at]
    m_new = m_old
    for t in range(2):
        m_new = jnp.maximum(m_new, top_ref[t : t + 1, at] - rows[t])
    weights = [
        jnp.exp2(s_ref[t * keys : (t + 1) * keys] - (m_new + rows[t])) for t in range(2)
    ]
    total = sum(jnp.sum(weight, axis=0, keepdims=True) for weight in weights)
    low = jnp.concatenate([weight.astype(BF16) for weight in weights], axis=0)
    shrink = jnp.exp2(m_old - m_new)
    l_ref[:, at] = l_ref[:, at] * shrink + total
    acc_ref[:, at] = acc_ref[:, at] * shrink + product(v, low, 0, 0)
    m_ref[:, at] = m_new


ORDER = (
    (0, 0, 2), (1, 0, 2), (2, 0, 2), (0, 2, 2), (1, 2, 2), (0, 4, 1), (1, 4, 1), (3, 0, 2),
    (2, 2, 1), (4, 0, 2), (2, 3, 1), (3, 2, 2), (2, 4, 1), (3, 4, 1), (4, 2, 1), (5, 0, 2),
    (4, 3, 1), (5, 2, 1), (4, 4, 1), (5, 3, 2),
)
STEP_LIST = [(unit, first + i) for unit, first, count in ORDER for i in range(count)]


def pair_at(p):
    code, start = p, 0
    for unit, first, count in ORDER:
        if start > 0:
            code = jnp.where(p >= start, p + (8 * unit + first - start), code)
        start += count
    return code // 8, lax.rem(code, 8)


def run_events(p, events, low, high):
    if not any(low <= at < high for at in events):
        return
    if high - low == 1:
        for act in events[low]:
            act()
        return
    middle = (low + high) // 2
    pl.when(p < middle)(lambda: run_events(p, events, low, middle))
    pl.when(p >= middle)(lambda: run_events(p, events, middle, high))


STEPS = 30


def layer_kernel(
    radius, q_ref, kv_ref, tk_ref, tv_ref, w_ref, out_ref,
    kvh, q2, m_ref, l_ref, acc_ref, top0, top1, s00, s01, s02, s10, s11, s12,
    ag, wg, part, part_far, leave, arrive,
    row_s, row_r, par_s, par_r, z_s, z_r, parcol_s, parcol_r, zcol_s, zcol_r,
    w_s, w_r, wf_s, wf_r, wl, ag_s, ag_r, agf_s, agf_r, end_s, end_r, sum_s, sum_r,
):
    heads = q_ref.shape[0]
    tokens = q_ref.shape[2]
    width = heads * HEAD
    half = width // 2
    ha, wa, hd = lax.axis_index("ha"), lax.axis_index("wa"), lax.axis_index("hd")
    last = lax.axis_size("wa") - 1
    core = lax.rem(ha, 2)
    partner = ha + 1 - 2 * core
    inner = (ha == 1) | (ha == 2)
    peer = 3 - ha
    x = lax.rem(hd, NX)
    z = hd // NX
    near = 2 - 2 * core
    far = 2 * core
    has_left, has_right = wa > 0, wa < last

    def x_at(step):
        return z * NX + lax.rem(x + step, NX)

    def remote(src, dst, send, recv, device):
        return pltpu.make_async_remote_copy(
            src_ref=src, dst_ref=dst, send_sem=send, recv_sem=recv,
            device_id=device, device_id_type=MESH,
        )

    def row_copy(h, side):
        return remote(
            kv_ref.at[h, 1 - side], kvh.at[h, 4 + 3 * side], row_s.at[h, side], row_r.at[h, side],
            {"wa": wa + 1 - 2 * side},
        )

    def par_copy(h):
        return remote(
            kv_ref.at[h], kvh.at[h, pl.ds(4 * far + 1, 2)], par_s.at[h], par_r.at[h], {"ha": partner}
        )

    def z_copy(h):
        return remote(
            kv_ref.at[h], kvh.at[h, pl.ds(4 * near + 1, 2)], z_s.at[h], z_r.at[h], {"ha": peer}
        )

    def parcol_copy(h, side):
        return remote(
            kvh.at[h, 4 + 3 * side], kvh.at[h, 4 * far + 3 * side],
            parcol_s.at[h, side], parcol_r.at[h, side], {"ha": partner},
        )

    def zcol_copy(h, side):
        return remote(
            kvh.at[h, 4 * far + 2 - side], kvh.at[h, 4 * far + 3 * side],
            zcol_s.at[h, side], zcol_r.at[h, side], {"wa": wa + 1 - 2 * side},
        )

    def w_copy(step, zc):
        cols = pl.multiple_of((zc * NX + lax.rem(x + step, NX)) * width, HEAD)
        return remote(
            w_ref.at[pl.ds(core * half, half), pl.ds(cols, width)],
            wg.at[zc, pl.ds(x * width + core * half, half)],
            w_s.at[step - 1, zc], w_r.at[step - 1, zc], {"hd": x_at(step)},
        )

    def w_forward(step, zc):
        rows = pl.ds(lax.rem(x + NX - step, NX) * width + core * half, half)
        return remote(
            wg.at[zc, rows], wg.at[zc, rows],
            wf_s.at[step - 1, zc], wf_r.at[step - 1, zc], {"ha": partner},
        )

    def w_own(zc):
        cols = pl.multiple_of((zc * NX + x) * width, HEAD)
        return pltpu.make_async_copy(
            w_ref.at[:, pl.ds(cols, width)], wg.at[zc, pl.ds(x * width, width)], wl.at[zc]
        )

    def ag_copy(c, h, way):
        return remote(
            ag.at[c, x, h], ag.at[c, x, h], ag_s.at[c, h, way], ag_r.at[c, h, way],
            {"hd": x_at(1 + 2 * way)},
        )

    def ag_forward(c, h):
        block = ag.at[c, lax.rem(x + NX - 1 + 2 * c, NX), h]
        return remote(
            block, block, agf_s.at[c, h], agf_r.at[c, h], {"hd": x_at(1 + 2 * c)}
        )

    def end_copy(c, b, hop):
        block = ag.at[c, x, heads - 1, pl.ds(b * SUB, SUB)]
        return remote(
            block, block, end_s.at[c, b, hop - 1], end_r.at[c, b, hop - 1], {"hd": x_at(hop)}
        )

    def sum_copy(c, b):
        at = pl.ds(b * SUB, SUB)
        return remote(
            leave.at[c, at], arrive.at[c, at], sum_s.at[c, b], sum_r.at[c, b],
            {"hd": lax.rem(hd + NX, 2 * NX)},
        )

    barrier = pltpu.get_barrier_semaphore()

    def greet(device):
        pl.semaphore_signal(barrier, inc=1, device_id=device, device_id_type=MESH)

    pl.when(has_left)(lambda: greet({"wa": wa - 1}))
    pl.when(has_right)(lambda: greet({"wa": wa + 1}))
    pl.when(inner)(lambda: greet({"ha": peer}))
    greet({"ha": partner})
    for step in range(1, NX):
        greet({"hd": x_at(step)})
    greet({"hd": lax.rem(hd + NX, 2 * NX)})
    def when_side(side, act):
        pl.when(has_right if side == 0 else has_left)(act)

    def when_from(side, act):
        pl.when(has_left if side == 0 else has_right)(act)

    def start_rows(h):
        for side in range(2):
            when_side(side, lambda side=side: row_copy(h, side).start())

    for h in range(heads):
        kvh[h, 5:7] = kv_ref[h]
        lanes = slice(h * HEAD, (h + 1) * HEAD)
        for copy in range(3):
            rows = slice(copy * SUB, (copy + 1) * SUB)
            kvh[h, TEXT_SLOT, 0, rows] = tk_ref[:, lanes]
            kvh[h, TEXT_SLOT, 1, rows] = tv_ref[:, lanes]
    for u in range(2 * heads):
        q = q_ref[u // 2, u % 2].astype(F32) * FACTOR
        q_high = q.astype(BF16)
        q2[u, :, :HEAD] = q_high
        q2[u, :, HEAD:] = (q - q_high.astype(F32)).astype(BF16)
    m_ref[...] = jnp.full_like(m_ref, -FAR)
    l_ref[...] = jnp.zeros_like(l_ref)
    acc_ref[...] = jnp.zeros_like(acc_ref)

    pl.semaphore_wait(
        barrier,
        2 + NX - 1
        + has_left.astype(jnp.int32) + has_right.astype(jnp.int32) + inner.astype(jnp.int32),
    )

    start_rows(0)
    for h in range(heads):
        pl.when(inner)(lambda h=h: z_copy(h).start())
        par_copy(h).start()
    for zc in range(2):
        w_own(zc).start()
        for step in (1, 3, 2):
            w_copy(step, zc).start()

    def serve_z(h):
        z_copy(h).wait_recv()
        for side in range(2):
            when_side(side, lambda side=side: zcol_copy(h, side).start())
        if h < heads - 1:
            start_rows(h + 1)

    def serve_rows(h):
        for side in range(2):

            @pl.when(has_left if side == 0 else has_right)
            def _(side=side):
                row_copy(h, side).wait_recv()
                parcol_copy(h, side).start()

    late = lax.broadcasted_iota(jnp.int32, (1, tokens), 1) >= tokens // 2
    sets = ((s00, s01, s02), (s10, s11, s12))
    peaks = (top0, top1)
    parts = tokens // SUB

    def halo_at(c):
        return jnp.where(c == 0, has_left.astype(jnp.int32), has_right.astype(jnp.int32))

    def chunk_at(c, chunk):
        v = chunk - 1
        side_col = v >= 6
        row_i = jnp.where(side_col, v - 6, v // 2)
        gap = jnp.where(side_col, 1, lax.rem(v, 2))
        there = ((row_i < 2) | inner) & ((v < 6) | (halo_at(c) > 0))
        row = jnp.where(row_i == 0, 1, jnp.where(row_i == 1, near, far))
        col = jnp.where(side_col, 3 * c, jnp.where(gap == 0, c + 1, 2 - c))
        slot = jnp.where(there, 4 * row + col, 5 + c)
        slot = jnp.where(chunk == 0, TEXT_SLOT, slot)
        return slot, there, (row_i > 0).astype(jnp.int32), gap

    def score_step(u, pair, which, part_i):
        slot, _, _, _ = chunk_at(lax.rem(u, 2), 2 * pair + which)
        score_part(q2.at[u], kvh[u // 2, slot, 0], part_i, sets[which][part_i], peaks[which])

    def pens_of(u, pair, which):
        c = lax.rem(u, 2)
        chunk = 2 * pair + which
        _, there, away, gap = chunk_at(c, chunk)
        pens = []
        for kt in range(2):
            pen = []
            for qt in range(2):
                ok = (
                    there
                    & (away <= radius[1, qt, 0, c])
                    & (gap <= radius[2, qt, 0, c])
                    & (abs(qt - kt) <= radius[0, qt, 0, c])
                )
                pen.append(jnp.where(chunk == 0, LOG3, jnp.where(ok, 0.0, FAR)))
            pens.append(jnp.where(late, pen[1], pen[0]))
        return pens

    def forward(u):
        h, c = u // 2, u % 2
        ag_copy(c, h, c).wait_recv()
        ag_forward(c, h).start()

    def rows_of(zc, h):
        return [wg[zc, i * width + h * HEAD : i * width + (h + 1) * HEAD] for i in range(NX)]

    def last_rows(zc):
        return jnp.concatenate(rows_of(zc, heads - 1), axis=0)

    def project_first(c):
        for h in range(heads - 1):
            ag_copy(c, h, 1 - c).wait_recv()
            ag_forward(c, h).wait_recv()
        for b in range(parts):
            at = slice(b * SUB, (b + 1) * SUB)
            lhs = jnp.concatenate(
                [ag[c, i, h, at] for h in range(heads - 1) for i in range(NX)], axis=1
            )
            for zc, out in ((1 - z, part_far), (z, part)):
                rhs = [block for h in range(heads - 1) for block in rows_of(zc, h)]
                out[c, at] = product(lhs, jnp.concatenate(rhs, axis=0), 1, 0)

    def project_last(c, b):
        for hop in (1, 3, 2):
            end_copy(c, b, hop).wait_recv()
        at = slice(b * SUB, (b + 1) * SUB)
        lhs = jnp.concatenate([ag[c, i, heads - 1, at] for i in range(NX)], axis=1)
        leave[c, at] = (part_far[c, at] + product(lhs, last_rows(1 - z), 1, 0)).astype(BF16)
        sum_copy(c, b).start()
        part[c, at] = part[c, at] + product(lhs, last_rows(z), 1, 0)

    for which in range(2):
        for part_i in range(parts):
            score_step(0, 0, which, part_i)

    events = {}

    def plan(at_step, act, *given):
        events.setdefault(at_step, []).append(lambda: act(*given))

    def await_pair(unit, pair):
        h, c = unit // 2, unit % 2
        if pair == 1 and c == 0:
            par_copy(h).wait_recv()
        if pair == 4:

            @pl.when(has_left if c == 0 else has_right)
            def _():
                parcol_copy(h, c).wait_recv()
                pl.when(inner)(lambda: zcol_copy(h, c).wait_recv())

    def pass_weights():
        for zc in range(2):
            for hop in (1, 3, 2):
                w_copy(hop, zc).wait_recv()
                w_forward(hop, zc).start()

    for at_step, h in ((5, 0), (12, 1), (18, 2)):
        plan(at_step, lambda h: pl.when(inner)(lambda: serve_z(h)), h)
    for at_step, h in ((8, 1), (17, 2)):
        plan(at_step, lambda h: pl.when(~inner)(lambda: start_rows(h)), h)
    for at_step, h in ((6, 0), (16, 1), (24, 2)):
        plan(at_step, serve_rows, h)
    plan(13, pass_weights)
    for at_step, done in ((18, 0), (23, 1), (28, 2)):
        plan(at_step, forward, done)
    for at_step, ahead in enumerate(STEP_LIST[1:]):
        if ahead[1] == 4 or (ahead[1] == 1 and ahead[0] % 2 == 0):
            plan(at_step, await_pair, *ahead)

    def step(p, carry):
        u, pair = carry
        u_next, pair_next = pair_at(jnp.minimum(p + 1, STEPS - 1))
        run_events(p, events, 0, STEPS)

        pens = [pens_of(u, pair, which) for which in range(2)]
        c, h = lax.rem(u, 2), u // 2
        for which in range(2):
            slot, _, _, _ = chunk_at(c, 2 * pair + which)
            for part_i in range(parts):
                blend_part(
                    kvh[h, slot, 1], pens[which], part_i, sets[which][part_i], peaks[which],
                    m_ref.at[u], l_ref.at[u], acc_ref.at[u],
                )
                score_step(u_next, pair_next, which, part_i)

        @pl.when((pair == 4) & (h < heads - 1))
        def _():
            ag[c, x, h] = (acc_ref[u] / l_ref[u]).T.astype(BF16)
            for way in range(2):
                ag_copy(c, h, way).start()

        @pl.when((pair == 4) & (h == heads - 1))
        def _():
            for b in range(parts):
                at = slice(b * SUB, (b + 1) * SUB)
                ag[c, x, heads - 1, at] = (acc_ref[u, :, at] / l_ref[u, :, at]).T.astype(BF16)
                for hop in (1, 3, 2):
                    end_copy(c, b, hop).start()

        return u_next, pair_next

    lax.fori_loop(0, STEPS, step, (jnp.int32(0), jnp.int32(0)))

    for zc in range(2):
        w_own(zc).wait()
        for hop in (1, 3, 2):
            w_forward(hop, zc).wait_recv()
    forward(3)
    project_first(0)
    project_last(0, 0)
    project_first(1)
    for b in range(1, parts):
        project_last(0, b)
    for b in range(parts):
        project_last(1, b)

    for c in range(2):
        for b in range(tokens // SUB):
            at = slice(b * SUB, (b + 1) * SUB)
            sum_copy(c, b).wait_recv()
            out_ref[c, at] = (part[c, at] + arrive[c, at].astype(F32)).astype(BF16)

    for c in range(2):
        for b in range(tokens // SUB):
            sum_copy(c, b).wait_send()
            for hop in range(1, NX):
                end_copy(c, b, hop).wait_send()
        for h in range(heads - 1):
            ag_forward(c, h).wait_send()
            for way in range(2):
                ag_copy(c, h, way).wait_send()
    for zc in range(2):
        for step in range(1, NX):
            w_copy(step, zc).wait_send()
            w_forward(step, zc).wait_send()
    for h in range(heads):
        par_copy(h).wait_send()
        pl.when(inner)(lambda h=h: z_copy(h).wait_send())
        for side in range(2):
            when_side(side, lambda h=h, side=side: row_copy(h, side).wait_send())
            when_from(side, lambda h=h, side=side: parcol_copy(h, side).wait_send())

            @pl.when(inner & (has_right if side == 0 else has_left))
            def _():
                zcol_copy(h, side).wait_send()


def layer(radius, q, kv, text_keys, text_values, out_weight):
    heads, cols, tokens, _ = q.shape
    width = heads * HEAD
    dma = pltpu.SemaphoreType.DMA
    vmem = pl.BlockSpec(memory_space=pltpu.VMEM)
    blocks = tokens // SUB
    return pl.pallas_call(
        layer_kernel,
        in_specs=[
            pl.BlockSpec(memory_space=pltpu.SMEM),
            vmem, vmem, vmem, vmem,
            pl.BlockSpec(memory_space=pl.ANY),
        ],
        out_specs=vmem,
        out_shape=jax.ShapeDtypeStruct((cols, tokens, width), BF16),
        scratch_shapes=[
            pltpu.VMEM((heads, TEXT_SLOT + 1, 2, tokens, HEAD), BF16),
            pltpu.VMEM((2 * heads, tokens, 2 * HEAD), BF16),
            pltpu.VMEM((2 * heads, 1, tokens), F32),
            pltpu.VMEM((2 * heads, 1, tokens), F32),
            pltpu.VMEM((2 * heads, HEAD, tokens), F32),
            pltpu.VMEM((2, tokens), F32),
            pltpu.VMEM((2, tokens), F32),
            *[pltpu.VMEM((tokens, SUB), F32)] * (2 * blocks),
            pltpu.VMEM((cols, NX, heads, tokens, HEAD), BF16),
            pltpu.VMEM((2, NX * width, width), BF16),
            pltpu.VMEM((cols, tokens, width), F32),
            pltpu.VMEM((cols, tokens, width), F32),
            pltpu.VMEM((cols, tokens, width), BF16),
            pltpu.VMEM((cols, tokens, width), BF16),
            dma((heads, 2)), dma((heads, 2)),
            dma((heads,)), dma((heads,)),
            dma((heads,)), dma((heads,)),
            dma((heads, 2)), dma((heads, 2)),
            dma((heads, 2)), dma((heads, 2)),
            dma((NX - 1, 2)), dma((NX - 1, 2)),
            dma((NX - 1, 2)), dma((NX - 1, 2)),
            dma((2,)),
            dma((cols, heads - 1, 2)), dma((cols, heads - 1, 2)),
            dma((cols, heads - 1)), dma((cols, heads - 1)),
            dma((cols, blocks, NX - 1)), dma((cols, blocks, NX - 1)),
            dma((cols, blocks)), dma((cols, blocks)),
        ],
        compiler_params=pltpu.CompilerParams(
            collective_id=0, has_side_effects=True, vmem_limit_bytes=60 * 1024 * 1024
        ),
        cost_estimate=pl.CostEstimate(
            flops=40_000_000_000, bytes_accessed=18_000_000, transcendentals=30_000_000
        ),
        name="layer",
    )(radius, q, kv, text_keys, text_values, out_weight)


def shards(queries, video_keys, video_values, text_keys, text_values, tile_radius, out_weight):
    n_frames, height, _, _ = queries.shape
    q = tiled(queries)
    kv = jnp.stack([tiled(video_keys), tiled(video_values)], axis=2)
    return untiled(layer(tile_radius, q, kv, text_keys, text_values, out_weight), n_frames, height)


def solution(mesh):
    placed = (
        P(None, "ha", "wa", "hd"),
        P(None, "ha", "wa", "hd"),
        P(None, "ha", "wa", "hd"),
        P(None, "hd"),
        P(None, "hd"),
        P(None, None, "ha", "wa"),
        P("hd", None),
    )
    return jax.shard_map(
        shards, mesh=mesh, in_specs=placed, out_specs=P(None, "ha", "wa", "hd"), check_vma=False
    )
```

```python
import functools

import jax
import jax.numpy as jnp
from jax import lax
from jax.experimental import pallas as pl
from jax.experimental.pallas import tpu as pltpu
from jax.sharding import PartitionSpec as P

HEAD = 128
TILE_W = 8
FACTOR = 1.4426950408889634 * HEAD ** (-0.5)
FAR = 1e30
LOG3 = 1.5849625007211562
TEXT_SLOT = 12
SUB = 256
NX = 4
BF16 = jnp.bfloat16
F32 = jnp.float32
MESH = pl.DeviceIdType.MESH


def tiled(block):
    frames, height, across, channels = block.shape
    cols = across // TILE_W
    heads = channels // HEAD
    cut = block.reshape(frames, height, cols, TILE_W, heads, HEAD)
    return cut.transpose(4, 2, 0, 1, 3, 5).reshape(heads, cols, -1, HEAD)


def untiled(tiles, frames, height):
    cols, _, channels = tiles.shape
    cut = tiles.reshape(cols, frames, height, TILE_W, channels)
    return cut.transpose(1, 2, 0, 3, 4).reshape(frames, height, cols * TILE_W, channels)


def product(a, b, over_a, over_b):
    return lax.dot_general(a, b, (((over_a,), (over_b,)), ((), ())), preferred_element_type=F32)


def score_part(q2, k, part, s_ref, top_ref):
    at = slice(part * SUB, (part + 1) * SUB)
    s = product(jnp.concatenate([k, k], axis=1), q2[at], 1, 1)
    s_ref[...] = s
    keys = k.shape[0] // 2
    for t in range(2):
        top_ref[t : t + 1, at] = jnp.max(s[t * keys : (t + 1) * keys], axis=0, keepdims=True)


def blend_part(v, pens, part, s_ref, top_ref, m_ref, l_ref, acc_ref):
    at = slice(part * SUB, (part + 1) * SUB)
    keys = v.shape[0] // 2
    rows = [pen[:, at] for pen in pens]
    m_old = m_ref[:, at]
    m_new = m_old
    for t in range(2):
        m_new = jnp.maximum(m_new, top_ref[t : t + 1, at] - rows[t])
    weights = [
        jnp.exp2(s_ref[t * keys : (t + 1) * keys] - (m_new + rows[t])) for t in range(2)
    ]
    total = sum(jnp.sum(weight, axis=0, keepdims=True) for weight in weights)
    low = jnp.concatenate([weight.astype(BF16) for weight in weights], axis=0)
    shrink = jnp.exp2(m_old - m_new)
    l_ref[:, at] = l_ref[:, at] * shrink + total
    acc_ref[:, at] = acc_ref[:, at] * shrink + product(v, low, 0, 0)
    m_ref[:, at] = m_new


ORDER = ((0, 0, 2), (1, 0, 2), (2, 0, 2), (0, 2, 2), (1, 2, 2), (0, 4, 1), (1, 4, 1), (3, 0, 2), (2, 2, 2), (3, 2, 2), (2, 4, 1), (3, 4, 1), (4, 0, 5), (5, 0, 5))
STEP_LIST = [(unit, first + i) for unit, first, count in ORDER for i in range(count)]


def pair_at(p):
    code, start = p, 0
    for unit, first, count in ORDER:
        if start > 0:
            code = jnp.where(p >= start, p + (8 * unit + first - start), code)
        start += count
    return code // 8, lax.rem(code, 8)


def run_events(p, events, low, high):
    if not any(low <= at < high for at in events):
        return
    if high - low == 1:
        for act in events[low]:
            act()
        return
    middle = (low + high) // 2
    pl.when(p < middle)(lambda: run_events(p, events, low, middle))
    pl.when(p >= middle)(lambda: run_events(p, events, middle, high))


STEPS = 30


def layer_kernel(
    radius, q_ref, kv_ref, tk_ref, tv_ref, w_ref, out_ref,
    kvh, q2, m_ref, l_ref, acc_ref, top0, top1, s00, s01, s02, s10, s11, s12,
    ag, wg, part, part_far, leave, arrive,
    row_s, row_r, par_s, par_r, z_s, z_r, parcol_s, parcol_r, zcol_s, zcol_r,
    w_s, w_r, wf_s, wf_r, wl, ag_s, ag_r, agf_s, agf_r, end_s, end_r, sum_s, sum_r,
):
    heads = q_ref.shape[0]
    tokens = q_ref.shape[2]
    width = heads * HEAD
    half = width // 2
    ha, wa, hd = lax.axis_index("ha"), lax.axis_index("wa"), lax.axis_index("hd")
    last = lax.axis_size("wa") - 1
    core = lax.rem(ha, 2)
    partner = ha + 1 - 2 * core
    inner = (ha == 1) | (ha == 2)
    peer = 3 - ha
    x = lax.rem(hd, NX)
    z = hd // NX
    near = 2 - 2 * core
    far = 2 * core
    has_left, has_right = wa > 0, wa < last

    def x_at(step):
        return z * NX + lax.rem(x + step, NX)

    def remote(src, dst, send, recv, device):
        return pltpu.make_async_remote_copy(
            src_ref=src, dst_ref=dst, send_sem=send, recv_sem=recv,
            device_id=device, device_id_type=MESH,
        )

    def row_copy(h, side):
        return remote(
            kv_ref.at[h, 1 - side], kvh.at[h, 4 + 3 * side], row_s.at[h, side], row_r.at[h, side],
            {"wa": wa + 1 - 2 * side},
        )

    def par_copy(h):
        return remote(
            kv_ref.at[h], kvh.at[h, pl.ds(4 * far + 1, 2)], par_s.at[h], par_r.at[h], {"ha": partner}
        )

    def z_copy(h):
        return remote(
            kv_ref.at[h], kvh.at[h, pl.ds(4 * near + 1, 2)], z_s.at[h], z_r.at[h], {"ha": peer}
        )

    def parcol_copy(h, side):
        return remote(
            kvh.at[h, 4 + 3 * side], kvh.at[h, 4 * far + 3 * side],
            parcol_s.at[h, side], parcol_r.at[h, side], {"ha": partner},
        )

    def zcol_copy(h, side):
        return remote(
            kvh.at[h, 4 * far + 2 - side], kvh.at[h, 4 * far + 3 * side],
            zcol_s.at[h, side], zcol_r.at[h, side], {"wa": wa + 1 - 2 * side},
        )

    def w_copy(step, zc):
        cols = pl.multiple_of((zc * NX + lax.rem(x + step, NX)) * width, HEAD)
        return remote(
            w_ref.at[pl.ds(core * half, half), pl.ds(cols, width)],
            wg.at[zc, pl.ds(x * width + core * half, half)],
            w_s.at[step - 1, zc], w_r.at[step - 1, zc], {"hd": x_at(step)},
        )

    def w_forward(step, zc):
        rows = pl.ds(lax.rem(x + NX - step, NX) * width + core * half, half)
        return remote(
            wg.at[zc, rows], wg.at[zc, rows],
            wf_s.at[step - 1, zc], wf_r.at[step - 1, zc], {"ha": partner},
        )

    def w_own(zc):
        cols = pl.multiple_of((zc * NX + x) * width, HEAD)
        return pltpu.make_async_copy(
            w_ref.at[:, pl.ds(cols, width)], wg.at[zc, pl.ds(x * width, width)], wl.at[zc]
        )

    def ag_copy(c, h, way):
        return remote(
            ag.at[c, x, h], ag.at[c, x, h], ag_s.at[c, h, way], ag_r.at[c, h, way],
            {"hd": x_at(1 + 2 * way)},
        )

    def ag_forward(c, h):
        block = ag.at[c, lax.rem(x + NX - 1 + 2 * c, NX), h]
        return remote(
            block, block, agf_s.at[c, h], agf_r.at[c, h], {"hd": x_at(1 + 2 * c)}
        )

    def end_copy(c, b, hop):
        block = ag.at[c, x, heads - 1, pl.ds(b * SUB, SUB)]
        return remote(
            block, block, end_s.at[c, b, hop - 1], end_r.at[c, b, hop - 1], {"hd": x_at(hop)}
        )

    def sum_copy(c, b):
        at = pl.ds(b * SUB, SUB)
        return remote(
            leave.at[c, at], arrive.at[c, at], sum_s.at[c, b], sum_r.at[c, b],
            {"hd": lax.rem(hd + NX, 2 * NX)},
        )

    barrier = pltpu.get_barrier_semaphore()

    def greet(device):
        pl.semaphore_signal(barrier, inc=1, device_id=device, device_id_type=MESH)

    pl.when(has_left)(lambda: greet({"wa": wa - 1}))
    pl.when(has_right)(lambda: greet({"wa": wa + 1}))
    pl.when(inner)(lambda: greet({"ha": peer}))
    greet({"ha": partner})
    for step in range(1, NX):
        greet({"hd": x_at(step)})
    greet({"hd": lax.rem(hd + NX, 2 * NX)})
    def when_side(side, act):
        pl.when(has_right if side == 0 else has_left)(act)

    def when_from(side, act):
        pl.when(has_left if side == 0 else has_right)(act)

    def start_rows(h):
        for side in range(2):
            when_side(side, lambda side=side: row_copy(h, side).start())

    for h in range(heads):
        kvh[h, 5:7] = kv_ref[h]
        lanes = slice(h * HEAD, (h + 1) * HEAD)
        for copy in range(3):
            rows = slice(copy * SUB, (copy + 1) * SUB)
            kvh[h, TEXT_SLOT, 0, rows] = tk_ref[:, lanes]
            kvh[h, TEXT_SLOT, 1, rows] = tv_ref[:, lanes]
    for u in range(2 * heads):
        q = q_ref[u // 2, u % 2].astype(F32) * FACTOR
        q_high = q.astype(BF16)
        q2[u, :, :HEAD] = q_high
        q2[u, :, HEAD:] = (q - q_high.astype(F32)).astype(BF16)
    m_ref[...] = jnp.full_like(m_ref, -FAR)
    l_ref[...] = jnp.zeros_like(l_ref)
    acc_ref[...] = jnp.zeros_like(acc_ref)

    pl.semaphore_wait(
        barrier,
        2 + NX - 1
        + has_left.astype(jnp.int32) + has_right.astype(jnp.int32) + inner.astype(jnp.int32),
    )

    start_rows(0)
    for h in range(heads):
        pl.when(inner)(lambda h=h: z_copy(h).start())
        par_copy(h).start()
    for zc in range(2):
        w_own(zc).start()
        for step in (1, 3, 2):
            w_copy(step, zc).start()

    def serve_z(h):
        z_copy(h).wait_recv()
        for side in range(2):
            when_side(side, lambda side=side: zcol_copy(h, side).start())
        if h < heads - 1:
            start_rows(h + 1)

    def serve_rows(h):
        for side in range(2):

            @pl.when(has_left if side == 0 else has_right)
            def _(side=side):
                row_copy(h, side).wait_recv()
                parcol_copy(h, side).start()

    late = lax.broadcasted_iota(jnp.int32, (1, tokens), 1) >= tokens // 2
    sets = ((s00, s01, s02), (s10, s11, s12))
    peaks = (top0, top1)
    parts = tokens // SUB

    def halo_at(c):
        return jnp.where(c == 0, has_left.astype(jnp.int32), has_right.astype(jnp.int32))

    def chunk_at(c, chunk):
        v = chunk - 1
        side_col = v >= 6
        row_i = jnp.where(side_col, v - 6, v // 2)
        gap = jnp.where(side_col, 1, lax.rem(v, 2))
        there = ((row_i < 2) | inner) & ((v < 6) | (halo_at(c) > 0))
        row = jnp.where(row_i == 0, 1, jnp.where(row_i == 1, near, far))
        col = jnp.where(side_col, 3 * c, jnp.where(gap == 0, c + 1, 2 - c))
        slot = jnp.where(there, 4 * row + col, 5 + c)
        slot = jnp.where(chunk == 0, TEXT_SLOT, slot)
        return slot, there, (row_i > 0).astype(jnp.int32), gap

    def score_step(u, pair, which, part_i):
        slot, _, _, _ = chunk_at(lax.rem(u, 2), 2 * pair + which)
        score_part(q2.at[u], kvh[u // 2, slot, 0], part_i, sets[which][part_i], peaks[which])

    def pens_of(u, pair, which):
        c = lax.rem(u, 2)
        chunk = 2 * pair + which
        _, there, away, gap = chunk_at(c, chunk)
        pens = []
        for kt in range(2):
            pen = []
            for qt in range(2):
                ok = (
                    there
                    & (away <= radius[1, qt, 0, c])
                    & (gap <= radius[2, qt, 0, c])
                    & (abs(qt - kt) <= radius[0, qt, 0, c])
                )
                pen.append(jnp.where(chunk == 0, LOG3, jnp.where(ok, 0.0, FAR)))
            pens.append(jnp.where(late, pen[1], pen[0]))
        return pens

    def forward(u):
        h, c = u // 2, u % 2
        ag_copy(c, h, c).wait_recv()
        ag_forward(c, h).start()

    def rows_of(zc, h):
        return [wg[zc, i * width + h * HEAD : i * width + (h + 1) * HEAD] for i in range(NX)]

    def last_rows(zc):
        return jnp.concatenate(rows_of(zc, heads - 1), axis=0)

    def project_first(c):
        for h in range(heads - 1):
            ag_copy(c, h, 1 - c).wait_recv()
            ag_forward(c, h).wait_recv()
        for b in range(parts):
            at = slice(b * SUB, (b + 1) * SUB)
            lhs = jnp.concatenate(
                [ag[c, i, h, at] for h in range(heads - 1) for i in range(NX)], axis=1
            )
            for zc, out in ((1 - z, part_far), (z, part)):
                rhs = [block for h in range(heads - 1) for block in rows_of(zc, h)]
                out[c, at] = product(lhs, jnp.concatenate(rhs, axis=0), 1, 0)

    def project_last(c, b):
        for hop in (1, 3, 2):
            end_copy(c, b, hop).wait_recv()
        at = slice(b * SUB, (b + 1) * SUB)
        lhs = jnp.concatenate([ag[c, i, heads - 1, at] for i in range(NX)], axis=1)
        leave[c, at] = (part_far[c, at] + product(lhs, last_rows(1 - z), 1, 0)).astype(BF16)
        sum_copy(c, b).start()
        part[c, at] = part[c, at] + product(lhs, last_rows(z), 1, 0)

    for which in range(2):
        for part_i in range(parts):
            score_step(0, 0, which, part_i)

    events = {}

    def plan(at_step, act, *given):
        events.setdefault(at_step, []).append(lambda: act(*given))

    def await_pair(unit, pair):
        h, c = unit // 2, unit % 2
        if pair == 1 and c == 0:
            par_copy(h).wait_recv()
        if pair == 4:

            @pl.when(has_left if c == 0 else has_right)
            def _():
                parcol_copy(h, c).wait_recv()
                pl.when(inner)(lambda: zcol_copy(h, c).wait_recv())

    def pass_weights():
        for zc in range(2):
            for hop in (1, 3, 2):
                w_copy(hop, zc).wait_recv()
                w_forward(hop, zc).start()

    for at_step, h in ((4, 0), (10, 1), (15, 2)):
        plan(at_step, lambda h: pl.when(inner)(lambda: serve_z(h)), h)
    for at_step, h in ((7, 1), (14, 2)):
        plan(at_step, lambda h: pl.when(~inner)(lambda: start_rows(h)), h)
    for at_step, h in ((5, 0), (14, 1), (21, 2)):
        plan(at_step, serve_rows, h)
    plan(12, pass_weights)
    for at_step, done in ((15, 0), (18, 1), (23, 2), (26, 3)):
        plan(at_step, forward, done)
    for at_step, ahead in enumerate(STEP_LIST[1:]):
        if ahead[1] == 4 or (ahead[1] == 1 and ahead[0] % 2 == 0):
            plan(at_step, await_pair, *ahead)

    def weights_here():
        for zc in range(2):
            w_own(zc).wait()
            for hop in (1, 3, 2):
                w_forward(hop, zc).wait_recv()
        project_first(0)

    plan(27, weights_here)
    plan(28, project_last, 0, 0)
    plan(29, project_last, 0, 1)

    def step(p, carry):
        u, pair = carry
        u_next, pair_next = pair_at(jnp.minimum(p + 1, STEPS - 1))
        run_events(p, events, 0, STEPS)

        pens = [pens_of(u, pair, which) for which in range(2)]
        c, h = lax.rem(u, 2), u // 2
        for which in range(2):
            slot, _, _, _ = chunk_at(c, 2 * pair + which)
            for part_i in range(parts):
                blend_part(
                    kvh[h, slot, 1], pens[which], part_i, sets[which][part_i], peaks[which],
                    m_ref.at[u], l_ref.at[u], acc_ref.at[u],
                )
                score_step(u_next, pair_next, which, part_i)

        @pl.when((pair == 4) & (h < heads - 1))
        def _():
            ag[c, x, h] = (acc_ref[u] / l_ref[u]).T.astype(BF16)
            for way in range(2):
                ag_copy(c, h, way).start()

        @pl.when((pair == 4) & (h == heads - 1))
        def _():
            for b in range(parts):
                at = slice(b * SUB, (b + 1) * SUB)
                ag[c, x, heads - 1, at] = (acc_ref[u, :, at] / l_ref[u, :, at]).T.astype(BF16)
                for hop in (1, 3, 2):
                    end_copy(c, b, hop).start()

        return u_next, pair_next

    lax.fori_loop(0, STEPS, step, (jnp.int32(0), jnp.int32(0)))

    project_last(0, 2)
    project_first(1)
    for b in range(parts):
        project_last(1, b)

    for c in range(2):
        for b in range(tokens // SUB):
            at = slice(b * SUB, (b + 1) * SUB)
            sum_copy(c, b).wait_recv()
            out_ref[c, at] = (part[c, at] + arrive[c, at].astype(F32)).astype(BF16)

    for c in range(2):
        for b in range(tokens // SUB):
            sum_copy(c, b).wait_send()
            for hop in range(1, NX):
                end_copy(c, b, hop).wait_send()
        for h in range(heads - 1):
            ag_forward(c, h).wait_send()
            for way in range(2):
                ag_copy(c, h, way).wait_send()
    for zc in range(2):
        for step in range(1, NX):
            w_copy(step, zc).wait_send()
            w_forward(step, zc).wait_send()
    for h in range(heads):
        par_copy(h).wait_send()
        pl.when(inner)(lambda h=h: z_copy(h).wait_send())
        for side in range(2):
            when_side(side, lambda h=h, side=side: row_copy(h, side).wait_send())
            when_from(side, lambda h=h, side=side: parcol_copy(h, side).wait_send())

            @pl.when(inner & (has_right if side == 0 else has_left))
            def _():
                zcol_copy(h, side).wait_send()


def layer(radius, q, kv, text_keys, text_values, out_weight):
    heads, cols, tokens, _ = q.shape
    width = heads * HEAD
    dma = pltpu.SemaphoreType.DMA
    vmem = pl.BlockSpec(memory_space=pltpu.VMEM)
    blocks = tokens // SUB
    return pl.pallas_call(
        layer_kernel,
        in_specs=[
            pl.BlockSpec(memory_space=pltpu.SMEM),
            vmem, vmem, vmem, vmem,
            pl.BlockSpec(memory_space=pl.ANY),
        ],
        out_specs=vmem,
        out_shape=jax.ShapeDtypeStruct((cols, tokens, width), BF16),
        scratch_shapes=[
            pltpu.VMEM((heads, TEXT_SLOT + 1, 2, tokens, HEAD), BF16),
            pltpu.VMEM((2 * heads, tokens, 2 * HEAD), BF16),
            pltpu.VMEM((2 * heads, 1, tokens), F32),
            pltpu.VMEM((2 * heads, 1, tokens), F32),
            pltpu.VMEM((2 * heads, HEAD, tokens), F32),
            pltpu.VMEM((2, tokens), F32),
            pltpu.VMEM((2, tokens), F32),
            *[pltpu.VMEM((tokens, SUB), F32)] * (2 * blocks),
            pltpu.VMEM((cols, NX, heads, tokens, HEAD), BF16),
            pltpu.VMEM((2, NX * width, width), BF16),
            pltpu.VMEM((cols, tokens, width), F32),
            pltpu.VMEM((cols, tokens, width), F32),
            pltpu.VMEM((cols, tokens, width), BF16),
            pltpu.VMEM((cols, tokens, width), BF16),
            dma((heads, 2)), dma((heads, 2)),
            dma((heads,)), dma((heads,)),
            dma((heads,)), dma((heads,)),
            dma((heads, 2)), dma((heads, 2)),
            dma((heads, 2)), dma((heads, 2)),
            dma((NX - 1, 2)), dma((NX - 1, 2)),
            dma((NX - 1, 2)), dma((NX - 1, 2)),
            dma((2,)),
            dma((cols, heads - 1, 2)), dma((cols, heads - 1, 2)),
            dma((cols, heads - 1)), dma((cols, heads - 1)),
            dma((cols, blocks, NX - 1)), dma((cols, blocks, NX - 1)),
            dma((cols, blocks)), dma((cols, blocks)),
        ],
        compiler_params=pltpu.CompilerParams(
            collective_id=0, has_side_effects=True, vmem_limit_bytes=60 * 1024 * 1024
        ),
        cost_estimate=pl.CostEstimate(
            flops=40_000_000_000, bytes_accessed=18_000_000, transcendentals=30_000_000
        ),
        name="layer",
    )(radius, q, kv, text_keys, text_values, out_weight)


def shards(queries, video_keys, video_values, text_keys, text_values, tile_radius, out_weight):
    n_frames, height, _, _ = queries.shape
    q = tiled(queries)
    kv = jnp.stack([tiled(video_keys), tiled(video_values)], axis=2)
    return untiled(layer(tile_radius, q, kv, text_keys, text_values, out_weight), n_frames, height)


def solution(mesh):
    placed = (
        P(None, "ha", "wa", "hd"),
        P(None, "ha", "wa", "hd"),
        P(None, "ha", "wa", "hd"),
        P(None, "hd"),
        P(None, "hd"),
        P(None, None, "ha", "wa"),
        P("hd", None),
    )
    return jax.shard_map(
        shards, mesh=mesh, in_specs=placed, out_specs=P(None, "ha", "wa", "hd"), check_vma=False
    )
```
